8 devices in a mesh: dp: 1 (over z), sp: 8 (over y, x, core).
Axes of the slice: x: 2, y: 2, z: 1, core: 2. Of those that a mesh axis runs over, the one named last changes fastest.
Arguments:
- x_in: bfloat16 [4096, 4096], P(('dp', 'sp'))
- w_in: bfloat16 [4096, 16768], replicated
- a_neg: float32 [128], replicated
- dt_bias: float32 [128], replicated
- d_skip: float32 [128], replicated
- w_out: bfloat16 [8192, 4096], replicated
Outputs:
- output: bfloat16 [4096, 4096], P(('dp', 'sp'))
All inputs are finite; a program needn't handle non-finite values.
Results may differ from the reference program's by a relative error of at most 0.00344.
Values are sent between devices in bfloat16 or wider.
A program may use at most 1 GiB of HBM per device.

```python
import jax
import jax.numpy as jnp
from jax import lax

D_MODEL = 4096
HEADS = 128
HEAD_DIM = 64
STATE_DIM = 128
TOKENS_DEV = 512
SEQ_LEN = 4096
SEG_LEN = 128

INNER_DIM = HEADS * HEAD_DIM
PROJ_DIM = 2 * INNER_DIM + 2 * STATE_DIM + HEADS


def setup_inputs(seed: int = 0, part: int = 0) -> dict:
    root_key = jax.random.key(seed)
    k_x, k_win, k_a, k_bias, k_skip, k_wout = jax.random.split(root_key, 6)
    x_in = jax.random.normal(jax.random.fold_in(k_x, part), (SEQ_LEN, D_MODEL), jnp.float32)
    col_scale = jnp.concatenate([
        jnp.full((2 * INNER_DIM,), 1.0, jnp.float32),
        jnp.full((2 * STATE_DIM,), (STATE_DIM * TOKENS_DEV) ** -0.25, jnp.float32),
        jnp.full((HEADS,), 0.5, jnp.float32),
    ]) * D_MODEL ** -0.5
    w_in = jax.random.normal(k_win, (D_MODEL, PROJ_DIM), jnp.float32) * col_scale
    a_neg = -jax.random.uniform(k_a, (HEADS,), jnp.float32, 0.15, 1.2) / TOKENS_DEV
    dt_bias = jax.random.uniform(k_bias, (HEADS,), jnp.float32, -1.0, 1.0)
    d_skip = jax.random.uniform(k_skip, (HEADS,), jnp.float32, 0.5, 1.5)
    w_out = jax.random.normal(k_wout, (INNER_DIM, D_MODEL), jnp.float32) * INNER_DIM ** -0.5
    return {"x_in": x_in.astype(jnp.bfloat16), "w_in": w_in.astype(jnp.bfloat16), "a_neg": a_neg,
            "dt_bias": dt_bias, "d_skip": d_skip, "w_out": w_out.astype(jnp.bfloat16)}


def reference(x_in, w_in, a_neg, dt_bias, d_skip, w_out):
    causal = jnp.arange(SEG_LEN)[:, None] >= jnp.arange(SEG_LEN)[None, :]
    mask_three = causal[:, :, None]

    def seg_step(h_prev, x_seg):
        projected = jnp.dot(x_seg, w_in, preferred_element_type=jnp.float32).astype(jnp.bfloat16)
        z_gate = projected[:, :INNER_DIM].astype(jnp.float32)
        x_heads = projected[:, INNER_DIM:2 * INNER_DIM].astype(jnp.float32).reshape(SEG_LEN, HEADS, HEAD_DIM)
        b_mat = projected[:, 2 * INNER_DIM:2 * INNER_DIM + STATE_DIM]
        c_mat = projected[:, 2 * INNER_DIM + STATE_DIM:2 * INNER_DIM + 2 * STATE_DIM]
        dt_vals = jax.nn.softplus(projected[:, 2 * INNER_DIM + 2 * STATE_DIM:].astype(jnp.float32) + dt_bias)
        log_cum = jnp.cumsum(dt_vals * a_neg, axis=0)
        scores = jnp.dot(c_mat, b_mat.T, preferred_element_type=jnp.float32)
        decay_mat = jnp.where(mask_three, jnp.exp(jnp.where(mask_three, log_cum[:, None, :] - log_cum[None, :, :], 0.0)), 0.0)
        g_mat = (scores[:, :, None] * decay_mat * dt_vals[None, :, :]).astype(jnp.bfloat16)
        y_intra = jnp.einsum("tsh,shp->thp", g_mat.astype(jnp.float32), x_heads)
        x_weighted = (x_heads * (jnp.exp(log_cum[-1] - log_cum) * dt_vals)[:, :, None]).astype(jnp.bfloat16)
        s_seg = jnp.einsum("shp,sn->hpn", x_weighted.astype(jnp.float32), b_mat.astype(jnp.float32))
        h_cast = h_prev.astype(jnp.bfloat16).astype(jnp.float32)
        y_state = jnp.einsum("tn,hpn->thp", c_mat.astype(jnp.float32), h_cast) * jnp.exp(log_cum)[:, :, None]
        y_all = y_intra + y_state + d_skip[None, :, None] * x_heads
        h_next = jnp.exp(log_cum[-1])[:, None, None] * h_prev + s_seg
        gated = (y_all.reshape(SEG_LEN, INNER_DIM) * jax.nn.silu(z_gate)).astype(jnp.bfloat16)
        y_seg = (x_seg.astype(jnp.float32) + jnp.dot(gated, w_out, preferred_element_type=jnp.float32)).astype(jnp.bfloat16)
        return h_next, y_seg

    h_zero = jnp.zeros((HEADS, HEAD_DIM, STATE_DIM), jnp.float32)
    h_last, y_segs = lax.scan(seg_step, h_zero, x_in.reshape(SEQ_LEN // SEG_LEN, SEG_LEN, D_MODEL))
    return y_segs.reshape(SEQ_LEN, D_MODEL)
```

```python
import jax
import jax.numpy as jnp
from jax import lax
from jax.experimental import pallas as pl
from jax.experimental.pallas import tpu as pltpu
from jax.sharding import PartitionSpec as P

SEG = 128
HEAD_DIM = 64
STATE = 128
TILE = 512
HALF = TILE // 2
TILE_HEADS = TILE // HEAD_DIM
LANES = 128
LAG_X = 8
LAG_Y = 14
LOG2E = 1.4426950408889634
MESH = pl.DeviceIdType.MESH
BF16 = jnp.bfloat16
F32 = jnp.float32


def dot32(a, b):
    return jnp.dot(a, b, preferred_element_type=F32)


def spread(v, pairs):
    rows = v.shape[0]
    low = lax.broadcasted_iota(jnp.int32, (rows, LANES), 1) < HEAD_DIM
    parts = []
    for p in range(pairs):
        left = jnp.broadcast_to(v[:, 2 * p:2 * p + 1], (rows, LANES))
        right = jnp.broadcast_to(v[:, 2 * p + 1:2 * p + 2], (rows, LANES))
        parts.append(jnp.where(low, left, right))
    return jnp.concatenate(parts, axis=1)


def lane_shift(v, first):
    return pltpu.roll(v, lax.rem(LANES - first, LANES), 1)


def project_kernel(x_ref, w_ref, wbc_ref, wdt_ref, an_ref, db_ref,
                   u_ref, xw_ref, bc_ref, bt_ref, gl_ref, qt_ref, dec_ref, hin_ref,
                   wst, lsend, lall, s_own, rc, sx, rx, sy, ry, rf,
                   lsem, lrem, csem, crem, xsem, xrem, ysem, yrem, fsem, frem):
    step = pl.program_id(0)
    me = lax.axis_index("sp")
    tokens = x_ref.shape[0]
    segs = tokens // SEG
    tiles = s_own.shape[0]
    core = lax.rem(me, 2)
    xpos = lax.rem(me // 2, 2)
    ypos = me // 4
    peer_core = me + 1 - 2 * core
    peer_x = me + 2 - 4 * xpos
    peer_y = me + 4 - 8 * ypos
    barrier = pltpu.get_barrier_semaphore()

    def other(k):
        return lax.rem(me + k, 8)

    def log_copy(k):
        return pltpu.make_async_remote_copy(
            src_ref=lsend, dst_ref=lall.at[me], send_sem=lsem.at[k - 1], recv_sem=lrem.at[me],
            device_id={"sp": other(k)}, device_id_type=MESH)

    def remote(src, dst, send, recv, target):
        return pltpu.make_async_remote_copy(
            src_ref=src, dst_ref=dst, send_sem=send, recv_sem=recv,
            device_id={"sp": target}, device_id_type=MESH)

    def core_copy(c):
        return remote(s_own.at[c, 1 - core], rc.at[c], csem.at[c], crem.at[c], peer_core)

    def x_copy(c):
        return remote(sx.at[c], rx.at[c], xsem.at[c], xrem.at[c], peer_x)

    def y_copy(c):
        return remote(sy.at[c], ry.at[c], ysem.at[c], yrem.at[c], peer_y)

    def final_copy(c):
        return remote(sy.at[c], rf.at[c], fsem.at[c], frem.at[c], peer_core)

    def at_lag(lag):
        return jnp.logical_and(step >= lag, step < tiles + lag)

    def decay_row(logs, c):
        first = c * TILE_HEADS + core * (TILE_HEADS // 2)
        return spread(lane_shift(jnp.exp(logs), first), 2)[:1]

    @pl.when(step == 0)
    def _():
        for k in range(1, 8):
            pl.semaphore_signal(barrier, inc=1, device_id={"sp": other(k)}, device_id_type=MESH)
        x = x_ref[...]
        bc = dot32(x, wbc_ref[...]).astype(BF16)
        bc_ref[...] = bc
        raw = dot32(x, wdt_ref[...]).astype(BF16).astype(F32) + db_ref[...]
        dt = jnp.maximum(raw, 0.0) + jnp.log1p(jnp.exp(-jnp.abs(raw)))
        logs = dt * an_ref[...]
        tri = (lax.broadcasted_iota(jnp.int32, (SEG, SEG), 0)
               >= lax.broadcasted_iota(jnp.int32, (SEG, SEG), 1)).astype(F32)
        total = jnp.zeros((1, LANES), F32)
        row = lax.broadcasted_iota(jnp.int32, (8, LANES), 0)
        dec = jnp.zeros((8, LANES), F32)
        for c in range(segs):
            rows = slice(c * SEG, (c + 1) * SEG)
            cum = jnp.dot(tri, logs[rows], precision=lax.Precision.HIGHEST, preferred_element_type=F32)
            last = cum[SEG - 1:SEG]
            wst[rows, :] = jnp.exp(last - cum) * dt[rows]
            gl_ref[rows, :] = cum * LOG2E
            qt_ref[rows, :] = jnp.transpose(cum * LOG2E - jnp.log2(dt[rows]))
            bt_ref[rows, :] = jnp.transpose(bc[rows, :STATE].astype(F32)).astype(BF16)
            dec = jnp.where(row == c, jnp.exp(last), dec)
            total = total + last
        dec_ref[...] = dec
        lsend[...] = jnp.broadcast_to(total, (8, LANES))

    @pl.when(step == 1)
    def _():
        pl.semaphore_wait(barrier, 7)
        for k in range(1, 8):
            log_copy(k).start()
        lall[me] = lsend[...]

    @pl.when(at_lag(1))
    def _():
        core_copy(step - 1).start()

    @pl.when(step == 2)
    def _():
        for k in range(1, 8):
            log_copy(k).wait_send()
            source = other(k)
            pltpu.make_async_remote_copy(
                src_ref=lsend, dst_ref=lall.at[source], send_sem=lsem.at[k - 1], recv_sem=lrem.at[source],
                device_id={"sp": source}, device_id_type=MESH).wait_recv()

    @pl.when(at_lag(2))
    def _():
        c = step - 2
        core_copy(c).wait()
        mine, got = s_own[c, core], rc[c]
        early = jnp.where(core == 0, mine, got)
        late = jnp.where(core == 0, got, mine)
        sx[c] = decay_row(lall[me - core + 1], c) * early + late

    @pl.when(at_lag(3))
    def _():
        x_copy(step - 3).start()

    @pl.when(at_lag(LAG_X))
    def _():
        c = step - LAG_X
        x_copy(c).wait()
        mine, got = sx[c], rx[c]
        early = jnp.where(xpos == 0, mine, got)
        late = jnp.where(xpos == 0, got, mine)
        chip = ypos * 4 + 2
        sy[c] = decay_row(lall[chip] + lall[chip + 1], c) * early + late

    @pl.when(at_lag(LAG_X + 1))
    def _():
        y_copy(step - LAG_X - 1).start()

    @pl.when(at_lag(LAG_Y))
    def _():
        c = step - LAG_Y
        y_copy(c).wait()
        chip = ypos * 4
        logs = jnp.where(xpos == 1, lall[chip] + lall[chip + 1], 0.0)
        before = jnp.where(xpos == 1, rx[c], 0.0) + jnp.where(ypos == 1, decay_row(logs, c) * ry[c], 0.0)
        first = jnp.where(core == 0, s_own[c, core], rc[c])
        after = decay_row(lall[me - core], c) * before + first
        sx[c] = jnp.where(core == 0, before, after)
        sy[c] = jnp.where(core == 0, after, before)

    @pl.when(at_lag(LAG_Y + 1))
    def _():
        final_copy(step - LAG_Y - 1).start()

    @pl.when(at_lag(LAG_Y + 2))
    def _():
        c = step - LAG_Y - 2
        final_copy(c).wait()
        mine, got = sx[c], rf[c]
        hin_ref[:, :HALF] = jnp.where(core == 0, mine, got)
        hin_ref[:, HALF:] = jnp.where(core == 0, got, mine)

    u = dot32(x_ref[...], w_ref[...]).astype(BF16)
    u_ref[...] = u

    @pl.when(step < tiles)
    def _():
        weights = lane_shift(wst[...], step * TILE_HEADS)
        dec = spread(lane_shift(dec_ref[...], step * TILE_HEADS), TILE_HEADS // 2)
        state = jnp.zeros((STATE, TILE), F32)
        for c in range(segs):
            rows = slice(c * SEG, (c + 1) * SEG)
            xw = (u_ref[rows, :].astype(F32) * spread(weights[rows], TILE_HEADS // 2)).astype(BF16)
            xw_ref[rows, :] = xw
            state = dec[c:c + 1] * state + dot32(bt_ref[rows, :], xw)
        s_own[step, 0] = state[:, :HALF]
        s_own[step, 1] = state[:, HALF:]


def mix_kernel(z_ref, xs_ref, xw_ref, h_ref, bc_ref, bt_ref, gl_ref, qt_ref, dec_ref, ds_ref, x_ref, wo_ref,
               out_ref, acc, gated, scores):
    group = pl.program_id(0)
    groups = pl.num_programs(0)
    tokens = x_ref.shape[0]
    segs = tokens // SEG

    @pl.when(group == 0)
    def _():
        acc[...] = x_ref[...].astype(F32)
        for c in range(segs):
            rows = slice(c * SEG, (c + 1) * SEG)
            scores[rows, :] = lax.dot_general(bc_ref[rows, STATE:], bc_ref[rows, :STATE],
                                              (((1,), (1,)), ((), ())), preferred_element_type=F32)

    first = group * TILE_HEADS
    gl = lane_shift(gl_ref[...], first)
    dec = spread(lane_shift(dec_ref[...], first), TILE_HEADS // 2)
    skip = spread(lane_shift(jnp.broadcast_to(ds_ref[...], (8, LANES)), first), TILE_HEADS // 2)[:1]
    causal = (lax.broadcasted_iota(jnp.int32, (SEG, SEG), 0)
              >= lax.broadcasted_iota(jnp.int32, (SEG, SEG), 1))
    low = lax.broadcasted_iota(jnp.int32, (SEG, LANES), 1) < HEAD_DIM
    zero = jnp.zeros((SEG, LANES), BF16)
    state = h_ref[...]
    for c in range(segs):
        rows = slice(c * SEG, (c + 1) * SEG)
        y_state = dot32(bc_ref[rows, STATE:], state.astype(BF16))
        if c < segs - 1:
            state = dec[c:c + 1] * state + dot32(bt_ref[rows, :], xw_ref[rows, :])
        q_rows = qt_ref[pl.ds(pl.multiple_of(c * SEG + first, TILE_HEADS), TILE_HEADS), :]
        sc = scores[rows, :]
        for p in range(TILE_HEADS // 2):
            cols = slice(p * LANES, (p + 1) * LANES)
            col_a = jnp.broadcast_to(gl[rows, 2 * p:2 * p + 1], (SEG, LANES))
            col_b = jnp.broadcast_to(gl[rows, 2 * p + 1:2 * p + 2], (SEG, LANES))
            g_a = jnp.where(causal, sc * jnp.exp2(col_a - q_rows[2 * p:2 * p + 1]), 0.0).astype(BF16)
            g_b = jnp.where(causal, sc * jnp.exp2(col_b - q_rows[2 * p + 1:2 * p + 2]), 0.0).astype(BF16)
            xp = xs_ref[rows, cols]
            rhs = jnp.concatenate([jnp.where(low, xp, zero), jnp.where(low, zero, xp)], axis=0)
            y = dot32(jnp.concatenate([g_a, g_b], axis=1), rhs)
            y = y + y_state[:, cols] * jnp.exp2(jnp.where(low, col_a, col_b)) + skip[:, cols] * xp.astype(F32)
            z = z_ref[rows, cols].astype(F32)
            gated[rows, cols] = (y * (z / (1.0 + jnp.exp(-z)))).astype(BF16)

    acc[...] += dot32(gated[...], wo_ref[...])

    @pl.when(group == groups - 1)
    def _():
        out_ref[...] = acc[...].astype(BF16)


def solution(mesh):
    row_spec = P(("dp", "sp"), None)

    def local_mixer(x_loc, w_in, a_neg, dt_bias, d_skip, w_out):
        tokens, d_model = x_loc.shape
        inner = w_out.shape[0]
        heads = a_neg.shape[0]
        tiles = inner // TILE
        segs = tokens // SEG
        assert mesh.shape["sp"] == 8 and heads == LANES and inner == heads * HEAD_DIM
        assert tiles >= LAG_Y + 2
        bc_at = 2 * inner // (2 * STATE)
        dt_at = (2 * inner + 2 * STATE) // heads

        def fixed(shape):
            return pl.BlockSpec(shape, lambda i: (0,) * len(shape), pipeline_mode=pl.Buffered(1))

        def whole(shape):
            return pl.BlockSpec(shape, lambda i: (0,) * len(shape))

        half = (tiles, STATE, HALF)
        sems = pltpu.SemaphoreType.DMA((tiles,))
        u, xw, bc, bt, gl, qt, dec, h_in = pl.pallas_call(
            project_kernel,
            grid=(2 * tiles,),
            out_shape=[
                jax.ShapeDtypeStruct((tokens, 2 * inner), BF16),
                jax.ShapeDtypeStruct((tokens, inner), BF16),
                jax.ShapeDtypeStruct((tokens, 2 * STATE), BF16),
                jax.ShapeDtypeStruct((segs * STATE, SEG), BF16),
                jax.ShapeDtypeStruct((tokens, heads), F32),
                jax.ShapeDtypeStruct((segs * heads, SEG), F32),
                jax.ShapeDtypeStruct((8, heads), F32),
                jax.ShapeDtypeStruct((STATE, inner), F32),
            ],
            in_specs=[
                fixed((tokens, d_model)),
                pl.BlockSpec((d_model, TILE), lambda i: (0, lax.rem(i + tiles, 2 * tiles))),
                pl.BlockSpec((d_model, 2 * STATE), lambda i: (0, bc_at), pipeline_mode=pl.Buffered(1)),
                pl.BlockSpec((d_model, heads), lambda i: (0, dt_at), pipeline_mode=pl.Buffered(1)),
                fixed((1, heads)), fixed((1, heads)),
            ],
            out_specs=[
                pl.BlockSpec((tokens, TILE), lambda i: (0, lax.rem(i + tiles, 2 * tiles))),
                pl.BlockSpec((tokens, TILE), lambda i: (0, jnp.minimum(i, tiles - 1))),
                whole((tokens, 2 * STATE)), whole((segs * STATE, SEG)), whole((tokens, heads)),
                whole((segs * heads, SEG)), whole((8, heads)),
                pl.BlockSpec((STATE, TILE), lambda i: (0, jnp.maximum(i - (LAG_Y + 2), 0))),
            ],
            scratch_shapes=[
                pltpu.VMEM((tokens, heads), F32),
                pltpu.VMEM((8, heads), F32),
                pltpu.VMEM((8, 8, heads), F32),
                pltpu.VMEM((tiles, 2, STATE, HALF), F32),
                pltpu.VMEM(half, F32), pltpu.VMEM(half, F32), pltpu.VMEM(half, F32),
                pltpu.VMEM(half, F32), pltpu.VMEM(half, F32), pltpu.VMEM(half, F32),
                pltpu.SemaphoreType.DMA((7,)), pltpu.SemaphoreType.DMA((8,)),
                sems, sems, sems, sems, sems, sems, sems, sems,
            ],
            compiler_params=pltpu.CompilerParams(
                dimension_semantics=("arbitrary",), collective_id=0, has_side_effects=True,
                vmem_limit_bytes=60 * 1024 * 1024),
            cost_estimate=pl.CostEstimate(flops=2 * tokens * d_model * w_in.shape[1],
                                          bytes_accessed=2 * w_in.size, transcendentals=0),
            name="project",
        )(x_loc, w_in, w_in, w_in, a_neg.reshape(1, heads), dt_bias.reshape(1, heads))

        return pl.pallas_call(
            mix_kernel,
            grid=(tiles,),
            out_shape=jax.ShapeDtypeStruct((tokens, d_model), BF16),
            in_specs=[
                pl.BlockSpec((tokens, TILE), lambda i: (0, i)),
                pl.BlockSpec((tokens, TILE), lambda i: (0, i + tiles)),
                pl.BlockSpec((tokens, TILE), lambda i: (0, i)),
                pl.BlockSpec((STATE, TILE), lambda i: (0, i)),
                fixed((tokens, 2 * STATE)), fixed((segs * STATE, SEG)), fixed((tokens, heads)),
                fixed((segs * heads, SEG)), fixed((8, heads)), fixed((1, heads)),
                fixed((tokens, d_model)),
                pl.BlockSpec((TILE, d_model), lambda i: (i, 0)),
            ],
            out_specs=pl.BlockSpec((tokens, d_model), lambda i: (0, 0)),
            scratch_shapes=[
                pltpu.VMEM((tokens, d_model), F32),
                pltpu.VMEM((tokens, TILE), BF16),
                pltpu.VMEM((tokens, SEG), F32),
            ],
            compiler_params=pltpu.CompilerParams(
                dimension_semantics=("arbitrary",), vmem_limit_bytes=60 * 1024 * 1024),
            cost_estimate=pl.CostEstimate(flops=2 * tokens * d_model * inner,
                                          bytes_accessed=2 * w_out.size, transcendentals=0),
            name="mix",
        )(u, u, xw, h_in, bc, bt, gl, qt, dec, d_skip.reshape(1, heads), x_loc, w_out)

    return jax.shard_map(local_mixer, mesh=mesh, in_specs=(row_spec, P(), P(), P(), P(), P()),
                         out_specs=row_spec, check_vma=False)
```

```python
import jax
import jax.numpy as jnp
from jax import lax
from jax.experimental import pallas as pl
from jax.experimental.pallas import tpu as pltpu
from jax.sharding import PartitionSpec as P

SEG = 128
HEAD_DIM = 64
STATE = 128
TILE = 512
HALF = TILE // 2
TILE_HEADS = TILE // HEAD_DIM
LANES = 128
LAG_X = 9
LAG_Y = 14
LOG2E = 1.4426950408889634
MESH = pl.DeviceIdType.MESH
BF16 = jnp.bfloat16
F32 = jnp.float32


def dot32(a, b):
    return jnp.dot(a, b, preferred_element_type=F32)


def spread(v, pairs):
    rows = v.shape[0]
    low = lax.broadcasted_iota(jnp.int32, (rows, LANES), 1) < HEAD_DIM
    parts = []
    for p in range(pairs):
        left = jnp.broadcast_to(v[:, 2 * p:2 * p + 1], (rows, LANES))
        right = jnp.broadcast_to(v[:, 2 * p + 1:2 * p + 2], (rows, LANES))
        parts.append(jnp.where(low, left, right))
    return jnp.concatenate(parts, axis=1)


def lane_shift(v, first):
    return pltpu.roll(v, lax.rem(LANES - first, LANES), 1)


def project_kernel(x_ref, w_ref, wbc_ref, wdt_ref, an_ref, db_ref,
                   u_ref, xw_ref, bc_ref, bt_ref, gl_ref, qt_ref, dec_ref, hin_ref,
                   wst, uprev, drow, lsend, lall, s_own, rc, sx, rx, sy, ry, rf,
                   lsem, lrem, csem, crem, xsem, xrem, ysem, yrem, fsem, frem):
    step = pl.program_id(0)
    me = lax.axis_index("sp")
    tokens = x_ref.shape[0]
    segs = tokens // SEG
    tiles = s_own.shape[0]
    core = lax.rem(me, 2)
    xpos = lax.rem(me // 2, 2)
    ypos = me // 4
    peer_core = me + 1 - 2 * core
    peer_x = me + 2 - 4 * xpos
    peer_y = me + 4 - 8 * ypos
    barrier = pltpu.get_barrier_semaphore()

    def other(k):
        return lax.rem(me + k, 8)

    def log_copy(k):
        return pltpu.make_async_remote_copy(
            src_ref=lsend, dst_ref=lall.at[me], send_sem=lsem.at[k - 1], recv_sem=lrem.at[me],
            device_id={"sp": other(k)}, device_id_type=MESH)

    def remote(src, dst, send, recv, target):
        return pltpu.make_async_remote_copy(
            src_ref=src, dst_ref=dst, send_sem=send, recv_sem=recv,
            device_id={"sp": target}, device_id_type=MESH)

    def core_copy(c):
        return remote(s_own.at[c, 1 - core], rc.at[c], csem.at[c], crem.at[c], peer_core)

    def x_copy(c):
        return remote(sx.at[c], rx.at[c], xsem.at[c], xrem.at[c], peer_x)

    def y_copy(c):
        return remote(sy.at[c], ry.at[c], ysem.at[c], yrem.at[c], peer_y)

    def final_copy(c):
        return remote(sy.at[c], rf.at[c], fsem.at[c], frem.at[c], peer_core)

    def at_lag(lag):
        return jnp.logical_and(step >= lag, step < tiles + lag)

    def state_half(h, tile):
        cols = slice(h * HALF, (h + 1) * HALF)
        first = tile * TILE_HEADS + h * (TILE_HEADS // 2)
        weights = lane_shift(wst[...], first)
        dec = spread(lane_shift(dec_ref[...], first), 2)
        parts = []
        for c in range(segs):
            rows = slice(c * SEG, (c + 1) * SEG)
            xw = (uprev[rows, cols].astype(F32) * spread(weights[rows], 2)).astype(BF16)
            xw_ref[rows, cols] = xw
            parts.append(xw)

        def finish():
            state = dot32(bt_ref[:SEG, :], parts[0])
            for c in range(1, segs):
                state = dec[c:c + 1] * state + dot32(bt_ref[c * SEG:(c + 1) * SEG, :], parts[c])
            s_own[tile, h] = state
        return finish

    def project_half(h):
        cols = slice(h * HALF, (h + 1) * HALF)
        u = dot32(x_ref[...], w_ref[:, cols]).astype(BF16)
        u_ref[:, cols] = u
        uprev[:, cols] = u

    @pl.when(step == 0)
    def _():
        for k in range(1, 8):
            pl.semaphore_signal(barrier, inc=1, device_id={"sp": other(k)}, device_id_type=MESH)
        x = x_ref[...]
        bc = dot32(x, wbc_ref[...]).astype(BF16)
        bc_ref[...] = bc
        raw = dot32(x, wdt_ref[...]).astype(BF16).astype(F32) + db_ref[...]
        dt = jnp.maximum(raw, 0.0) + jnp.log1p(jnp.exp(-jnp.abs(raw)))
        logs = dt * an_ref[...]
        tri = (lax.broadcasted_iota(jnp.int32, (SEG, SEG), 0)
               >= lax.broadcasted_iota(jnp.int32, (SEG, SEG), 1)).astype(F32)
        total = jnp.zeros((1, LANES), F32)
        row = lax.broadcasted_iota(jnp.int32, (8, LANES), 0)
        dec = jnp.zeros((8, LANES), F32)
        for c in range(segs):
            rows = slice(c * SEG, (c + 1) * SEG)
            cum = jnp.dot(tri, logs[rows], precision=lax.Precision.HIGHEST, preferred_element_type=F32)
            last = cum[SEG - 1:SEG]
            wst[rows, :] = jnp.exp(last - cum) * dt[rows]
            gl_ref[rows, :] = cum * LOG2E
            qt_ref[rows, :] = jnp.transpose(cum * LOG2E - jnp.log2(dt[rows]))
            bt_ref[rows, :] = jnp.transpose(bc[rows, :STATE].astype(F32)).astype(BF16)
            dec = jnp.where(row == c, jnp.exp(last), dec)
            total = total + last
        dec_ref[...] = dec
        lsend[...] = jnp.broadcast_to(total, (8, LANES))

    def s_of(mine, c):
        return jnp.where(mine, s_own[c, core], rc[c])

    @pl.when(step == 1)
    def _():
        pl.semaphore_wait(barrier, 7)
        for k in range(1, 8):
            log_copy(k).start()
        lall[me] = lsend[...]

    @pl.when(at_lag(2))
    def _():
        core_copy(step - 2).start()

    @pl.when(step == 2)
    def _():
        for k in range(1, 8):
            log_copy(k).wait_send()
            source = other(k)
            pltpu.make_async_remote_copy(
                src_ref=lsend, dst_ref=lall.at[source], send_sem=lsem.at[k - 1], recv_sem=lrem.at[source],
                device_id={"sp": source}, device_id_type=MESH).wait_recv()
        chip = ypos * 4
        row = lax.broadcasted_iota(jnp.int32, (8, LANES), 0)
        logs = jnp.where(row == 0, lall[me - core + 1], 0.0)
        logs = jnp.where(row == 1, lall[chip + 2] + lall[chip + 3], logs)
        logs = jnp.where(jnp.logical_and(row == 2, xpos == 1), lall[chip] + lall[chip + 1], logs)
        logs = jnp.where(row == 3, lall[me - core], logs)
        decays = jnp.exp(logs)
        for c in range(tiles):
            drow[c] = spread(lane_shift(decays, c * TILE_HEADS + core * (TILE_HEADS // 2)), 2)

    @pl.when(at_lag(3))
    def _():
        c = step - 3
        core_copy(c).wait()
        sx[c] = drow[c, 0:1] * s_of(core == 0, c) + s_of(core == 1, c)

    @pl.when(at_lag(4))
    def _():
        x_copy(step - 4).start()

    @pl.when(at_lag(LAG_X))
    def _():
        c = step - LAG_X
        x_copy(c).wait()
        mine, got = sx[c], rx[c]
        early = jnp.where(xpos == 0, mine, got)
        late = jnp.where(xpos == 0, got, mine)
        sy[c] = drow[c, 1:2] * early + late

    @pl.when(at_lag(LAG_X + 1))
    def _():
        y_copy(step - LAG_X - 1).start()

    @pl.when(at_lag(LAG_Y))
    def _():
        c = step - LAG_Y
        y_copy(c).wait()
        before = jnp.where(xpos == 1, rx[c], 0.0) + jnp.where(ypos == 1, drow[c, 2:3] * ry[c], 0.0)
        after = drow[c, 3:4] * before + s_of(core == 0, c)
        sx[c] = jnp.where(core == 0, before, after)
        sy[c] = jnp.where(core == 0, after, before)

    @pl.when(at_lag(LAG_Y + 1))
    def _():
        final_copy(step - LAG_Y - 1).start()

    @pl.when(at_lag(LAG_Y + 2))
    def _():
        c = step - LAG_Y - 2
        final_copy(c).wait()
        mine, got = sx[c], rf[c]
        hin_ref[:, :HALF] = jnp.where(core == 0, mine, got)
        hin_ref[:, HALF:] = jnp.where(core == 0, got, mine)

    with_state = jnp.logical_and(step >= 1, step <= tiles)

    @pl.when(with_state)
    def _():
        for h in range(2):
            finish = state_half(h, step - 1)
            project_half(h)
            finish()

    @pl.when(jnp.logical_not(with_state))
    def _():
        for h in range(2):
            project_half(h)


def mix_kernel(z_ref, xs_ref, xw_ref, h_ref, bc_ref, bt_ref, gl_ref, qt_ref, dec_ref, ds_ref, wa_ref, wb_ref, x_hbm,
               out_ref, acc, gated_a, gated_b, scores, x_res, x_sem):
    step = pl.program_id(0)
    steps = pl.num_programs(0)
    tokens, d_model = acc.shape
    segs = tokens // SEG
    x_copy = pltpu.make_async_copy(x_hbm, x_res, x_sem)

    def dot_slice(k, source, w_ref):
        cols = slice(k * TILE, (k + 1) * TILE)
        acc[:, cols] += dot32(source[...], w_ref[:, cols])

    def group_outputs(half, target, big):
        base = half * TILE
        first = (2 * step + half) * TILE_HEADS
        gl = lane_shift(gl_ref[...], first)
        dec = spread(lane_shift(dec_ref[...], first), TILE_HEADS // 2)
        skip = spread(lane_shift(jnp.broadcast_to(ds_ref[...], (8, LANES)), first), TILE_HEADS // 2)[:1]
        causal = (lax.broadcasted_iota(jnp.int32, (SEG, SEG), 0)
                  >= lax.broadcasted_iota(jnp.int32, (SEG, SEG), 1))
        low = lax.broadcasted_iota(jnp.int32, (SEG, LANES), 1) < HEAD_DIM
        zero = jnp.zeros((SEG, LANES), BF16)
        state = h_ref[:, base:base + TILE]
        pending = None
        unit = 0
        for c in range(segs):
            rows = slice(c * SEG, (c + 1) * SEG)
            y_state = dot32(bc_ref[rows, STATE:], state.astype(BF16))
            if c < segs - 1:
                grown = dot32(bt_ref[rows, :], xw_ref[rows, base:base + TILE])
            q_rows = qt_ref[pl.ds(pl.multiple_of(c * SEG + first, TILE_HEADS), TILE_HEADS), :]
            for p in range(TILE_HEADS // 2):
                cols = slice(base + p * LANES, base + (p + 1) * LANES)
                sc = scores[rows, :]
                col_a = jnp.broadcast_to(gl[rows, 2 * p:2 * p + 1], (SEG, LANES))
                col_b = jnp.broadcast_to(gl[rows, 2 * p + 1:2 * p + 2], (SEG, LANES))
                g_a = jnp.where(causal, sc * jnp.exp2(col_a - q_rows[2 * p:2 * p + 1]), 0.0).astype(BF16)
                g_b = jnp.where(causal, sc * jnp.exp2(col_b - q_rows[2 * p + 1:2 * p + 2]), 0.0).astype(BF16)
                xp = xs_ref[rows, cols]
                rhs = jnp.concatenate([jnp.where(low, xp, zero), jnp.where(low, zero, xp)], axis=0)
                if unit % 2 == 0 and big is not None:
                    dot_slice(unit // 2, *big)
                y = dot32(jnp.concatenate([g_a, g_b], axis=1), rhs)
                if pending is not None:
                    pending()

                def pending(y=y, rows=rows, cols=cols, p=p, y_state=y_state, col_a=col_a, col_b=col_b):
                    here = slice(p * LANES, (p + 1) * LANES)
                    total = y + y_state[:, here] * jnp.exp2(jnp.where(low, col_a, col_b))
                    total = total + skip[:, here] * xs_ref[rows, cols].astype(F32)
                    z = z_ref[rows, cols].astype(F32)
                    target[rows, here] = (total * (z / (1.0 + jnp.exp(-z)))).astype(BF16)
                unit += 1
            if c < segs - 1:
                state = dec[c:c + 1] * state + grown
        pending()

    @pl.when(step == 0)
    def _():
        x_copy.start()
        acc[...] = jnp.zeros_like(acc)
        for c in range(segs):
            rows = slice(c * SEG, (c + 1) * SEG)
            scores[rows, :] = lax.dot_general(bc_ref[rows, STATE:], bc_ref[rows, :STATE],
                                              (((1,), (1,)), ((), ())), preferred_element_type=F32)
        group_outputs(0, gated_a, None)

    @pl.when(jnp.logical_and(step > 0, step < steps - 1))
    def _():
        group_outputs(0, gated_a, (gated_b, wa_ref))

    @pl.when(step < steps - 1)
    def _():
        group_outputs(1, gated_b, (gated_a, wb_ref))

    @pl.when(step == steps - 1)
    def _():
        x_copy.wait()
        for k in range(d_model // TILE):
            cols = slice(k * TILE, (k + 1) * TILE)
            total = acc[:, cols] + dot32(gated_b[...], wa_ref[:, cols])
            out_ref[:, cols] = (x_res[:, cols].astype(F32) + total).astype(BF16)


def solution(mesh):
    row_spec = P(("dp", "sp"), None)

    def local_mixer(x_loc, w_in, a_neg, dt_bias, d_skip, w_out):
        tokens, d_model = x_loc.shape
        inner = w_out.shape[0]
        heads = a_neg.shape[0]
        tiles = inner // TILE
        segs = tokens // SEG
        assert mesh.shape["sp"] == 8 and heads == LANES and inner == heads * HEAD_DIM
        assert tiles >= LAG_Y + 2
        bc_at = 2 * inner // (2 * STATE)
        dt_at = (2 * inner + 2 * STATE) // heads

        def fixed(shape):
            return pl.BlockSpec(shape, lambda i: (0,) * len(shape), pipeline_mode=pl.Buffered(1))

        def whole(shape):
            return pl.BlockSpec(shape, lambda i: (0,) * len(shape))

        half = (tiles, STATE, HALF)
        sems = pltpu.SemaphoreType.DMA((tiles,))
        u, xw, bc, bt, gl, qt, dec, h_in = pl.pallas_call(
            project_kernel,
            grid=(2 * tiles,),
            out_shape=[
                jax.ShapeDtypeStruct((tokens, 2 * inner), BF16),
                jax.ShapeDtypeStruct((tokens, inner), BF16),
                jax.ShapeDtypeStruct((tokens, 2 * STATE), BF16),
                jax.ShapeDtypeStruct((segs * STATE, SEG), BF16),
                jax.ShapeDtypeStruct((tokens, heads), F32),
                jax.ShapeDtypeStruct((segs * heads, SEG), F32),
                jax.ShapeDtypeStruct((8, heads), F32),
                jax.ShapeDtypeStruct((STATE, inner), F32),
            ],
            in_specs=[
                fixed((tokens, d_model)),
                pl.BlockSpec((d_model, TILE), lambda i: (0, lax.rem(i + tiles, 2 * tiles))),
                pl.BlockSpec((d_model, 2 * STATE), lambda i: (0, bc_at), pipeline_mode=pl.Buffered(1)),
                pl.BlockSpec((d_model, heads), lambda i: (0, dt_at), pipeline_mode=pl.Buffered(1)),
                fixed((1, heads)), fixed((1, heads)),
            ],
            out_specs=[
                pl.BlockSpec((tokens, TILE), lambda i: (0, lax.rem(i + tiles, 2 * tiles))),
                pl.BlockSpec((tokens, TILE), lambda i: (0, jnp.clip(i - 1, 0, tiles - 1))),
                whole((tokens, 2 * STATE)), whole((segs * STATE, SEG)), whole((tokens, heads)),
                whole((segs * heads, SEG)), whole((8, heads)),
                pl.BlockSpec((STATE, TILE), lambda i: (0, jnp.maximum(i - (LAG_Y + 2), 0))),
            ],
            scratch_shapes=[
                pltpu.VMEM((tokens, heads), F32),
                pltpu.VMEM((tokens, TILE), BF16),
                pltpu.VMEM((tiles, 8, HALF), F32),
                pltpu.VMEM((8, heads), F32),
                pltpu.VMEM((8, 8, heads), F32),
                pltpu.VMEM((tiles, 2, STATE, HALF), F32),
                pltpu.VMEM(half, F32), pltpu.VMEM(half, F32), pltpu.VMEM(half, F32),
                pltpu.VMEM(half, F32), pltpu.VMEM(half, F32), pltpu.VMEM(half, F32),
                pltpu.SemaphoreType.DMA((7,)), pltpu.SemaphoreType.DMA((8,)),
                sems, sems, sems, sems, sems, sems, sems, sems,
            ],
            compiler_params=pltpu.CompilerParams(
                dimension_semantics=("arbitrary",), collective_id=0, has_side_effects=True,
                vmem_limit_bytes=60 * 1024 * 1024),
            cost_estimate=pl.CostEstimate(flops=2 * tokens * d_model * w_in.shape[1],
                                          bytes_accessed=2 * w_in.size, transcendentals=0),
            name="project",
        )(x_loc, w_in, w_in, w_in, a_neg.reshape(1, heads), dt_bias.reshape(1, heads))

        last = tiles // 2 - 1
        return pl.pallas_call(
            mix_kernel,
            grid=(tiles // 2 + 1,),
            out_shape=jax.ShapeDtypeStruct((tokens, d_model), BF16),
            in_specs=[
                pl.BlockSpec((tokens, 2 * TILE), lambda i: (0, jnp.minimum(i, last))),
                pl.BlockSpec((tokens, 2 * TILE), lambda i: (0, jnp.minimum(i, last) + tiles // 2)),
                pl.BlockSpec((tokens, 2 * TILE), lambda i: (0, jnp.minimum(i, last))),
                pl.BlockSpec((STATE, 2 * TILE), lambda i: (0, jnp.minimum(i, last))),
                fixed((tokens, 2 * STATE)), fixed((segs * STATE, SEG)), fixed((tokens, heads)),
                fixed((segs * heads, SEG)), fixed((8, heads)), fixed((1, heads)),
                pl.BlockSpec((TILE, d_model), lambda i: (jnp.maximum(2 * i - 1, 0), 0)),
                pl.BlockSpec((TILE, d_model), lambda i: (jnp.minimum(2 * i, tiles - 2), 0)),
                pl.BlockSpec(memory_space=pl.ANY),
            ],
            out_specs=pl.BlockSpec((tokens, d_model), lambda i: (0, 0), pipeline_mode=pl.Buffered(1)),
            scratch_shapes=[
                pltpu.VMEM((tokens, d_model), F32),
                pltpu.VMEM((tokens, TILE), BF16),
                pltpu.VMEM((tokens, TILE), BF16),
                pltpu.VMEM((tokens, SEG), F32),
                pltpu.VMEM((tokens, d_model), BF16),
                pltpu.SemaphoreType.DMA(()),
            ],
            compiler_params=pltpu.CompilerParams(
                dimension_semantics=("arbitrary",), vmem_limit_bytes=62 * 1024 * 1024),
            cost_estimate=pl.CostEstimate(flops=2 * tokens * d_model * inner,
                                          bytes_accessed=2 * w_out.size, transcendentals=0),
            name="mix",
        )(u, u, xw, h_in, bc, bt, gl, qt, dec, d_skip.reshape(1, heads), w_out, w_out, x_loc)

    return jax.shard_map(local_mixer, mesh=mesh, in_specs=(row_spec, P(), P(), P(), P(), P()),
                         out_specs=row_spec, check_vma=False)
```

```python
import jax
import jax.numpy as jnp
from jax import lax
from jax.experimental import pallas as pl
from jax.experimental.pallas import tpu as pltpu
from jax.sharding import PartitionSpec as P

SEG = 128
HEAD_DIM = 64
STATE = 128
TILE = 512
HALF = TILE // 2
TILE_HEADS = TILE // HEAD_DIM
LANES = 128
LAG_X = 9
LAG_Y = 14
LOG2E = 1.4426950408889634
MESH = pl.DeviceIdType.MESH
BF16 = jnp.bfloat16
F32 = jnp.float32


def dot32(a, b):
    return jnp.dot(a, b, preferred_element_type=F32)


def spread(v, pairs):
    rows = v.shape[0]
    low = lax.broadcasted_iota(jnp.int32, (rows, LANES), 1) < HEAD_DIM
    parts = []
    for p in range(pairs):
        left = jnp.broadcast_to(v[:, 2 * p:2 * p + 1], (rows, LANES))
        right = jnp.broadcast_to(v[:, 2 * p + 1:2 * p + 2], (rows, LANES))
        parts.append(jnp.where(low, left, right))
    return jnp.concatenate(parts, axis=1)


def lane_shift(v, first):
    return pltpu.roll(v, lax.rem(LANES - first, LANES), 1)


def project_kernel(x_hbm, w_ref, w_hbm, an_hbm, db_hbm,
                   u_ref, loc_ref, hin_ref, bc_hbm, gl_hbm, qt_hbm, dec_hbm,
                   x_ref, wbc_ref, wdt_ref, an_ref, db_ref, bc_ref, gl_ref, qt_ref, dec_ref, isem, osem,
                   bt_ref, seg_dec, xw_ref, wst, uprev, drow, lsend, lall, s_own, rc, sx, rx, sy, ry, rf,
                   lsem, lrem, csem, crem, xsem, xrem, ysem, yrem, fsem, frem):
    step = pl.program_id(0)
    me = lax.axis_index("sp")
    tokens = x_ref.shape[0]
    segs = tokens // SEG
    tiles = s_own.shape[0]
    heads_at = 2 * tiles * TILE
    loads = [
        pltpu.make_async_copy(db_hbm, db_ref, isem.at[0]),
        pltpu.make_async_copy(an_hbm, an_ref, isem.at[1]),
        pltpu.make_async_copy(w_hbm.at[:, heads_at + 2 * STATE:], wdt_ref, isem.at[2]),
        pltpu.make_async_copy(x_hbm, x_ref, isem.at[3]),
        pltpu.make_async_copy(w_hbm.at[:, heads_at:heads_at + 2 * STATE], wbc_ref, isem.at[4]),
    ]
    stores = [
        pltpu.make_async_copy(bc_ref, bc_hbm, osem.at[0]),
        pltpu.make_async_copy(gl_ref, gl_hbm, osem.at[1]),
        pltpu.make_async_copy(qt_ref, qt_hbm, osem.at[2]),
        pltpu.make_async_copy(dec_ref, dec_hbm, osem.at[3]),
    ]
    core = lax.rem(me, 2)
    xpos = lax.rem(me // 2, 2)
    ypos = me // 4
    peer_core = me + 1 - 2 * core
    peer_x = me + 2 - 4 * xpos
    peer_y = me + 4 - 8 * ypos
    barrier = pltpu.get_barrier_semaphore()

    def other(k):
        return lax.rem(me + k, 8)

    def log_copy(k):
        return pltpu.make_async_remote_copy(
            src_ref=lsend, dst_ref=lall.at[me], send_sem=lsem.at[k - 1], recv_sem=lrem.at[me],
            device_id={"sp": other(k)}, device_id_type=MESH)

    def remote(src, dst, send, recv, target):
        return pltpu.make_async_remote_copy(
            src_ref=src, dst_ref=dst, send_sem=send, recv_sem=recv,
            device_id={"sp": target}, device_id_type=MESH)

    def core_copy(c):
        return remote(s_own.at[c, 1 - core], rc.at[c], csem.at[c], crem.at[c], peer_core)

    def x_copy(c):
        return remote(sx.at[c], rx.at[c], xsem.at[c], xrem.at[c], peer_x)

    def y_copy(c):
        return remote(sy.at[c], ry.at[c], ysem.at[c], yrem.at[c], peer_y)

    def final_copy(c):
        return remote(sy.at[c], rf.at[c], fsem.at[c], frem.at[c], peer_core)

    def at_lag(lag):
        return jnp.logical_and(step >= lag, step < tiles + lag)

    def weigh(tile):
        weights = lane_shift(wst[...], tile * TILE_HEADS)
        for c in range(segs):
            rows = slice(c * SEG, (c + 1) * SEG)
            spread_rows = spread(weights[rows], TILE_HEADS // 2)
            xw_ref[rows, :] = (uprev[rows, :].astype(F32) * spread_rows).astype(BF16)

    def states(tile):
        dec = spread(lane_shift(seg_dec[...], tile * TILE_HEADS), TILE_HEADS // 2)
        state = dot32(bt_ref[:SEG, :], xw_ref[:SEG, :])
        for c in range(1, segs):
            rows = slice(c * SEG, (c + 1) * SEG)
            loc_ref[(c - 1) * STATE:c * STATE, :] = state
            state = dec[c:c + 1] * state + dot32(bt_ref[rows, :], xw_ref[rows, :])
        s_own[tile, 0] = state[:, :HALF]
        s_own[tile, 1] = state[:, HALF:]

    def project_half(h):
        cols = slice(h * HALF, (h + 1) * HALF)
        u = dot32(x_ref[...], w_ref[:, cols]).astype(BF16)
        u_ref[:, cols] = u
        uprev[:, cols] = u

    @pl.when(step == 0)
    def _():
        for k in range(1, 8):
            pl.semaphore_signal(barrier, inc=1, device_id={"sp": other(k)}, device_id_type=MESH)
        for load in loads:
            load.start()
        for load in loads[:4]:
            load.wait()
        raw = dot32(x_ref[...], wdt_ref[...]).astype(BF16).astype(F32) + db_ref[...]
        loads[4].wait()
        bc = dot32(x_ref[...], wbc_ref[...]).astype(BF16)
        bc_ref[...] = bc
        dt = jnp.maximum(raw, 0.0) + jnp.log1p(jnp.exp(-jnp.abs(raw)))
        logs = dt * an_ref[...]
        tri = (lax.broadcasted_iota(jnp.int32, (SEG, SEG), 0)
               >= lax.broadcasted_iota(jnp.int32, (SEG, SEG), 1)).astype(F32)
        total = jnp.zeros((1, LANES), F32)
        row = lax.broadcasted_iota(jnp.int32, (8, LANES), 0)
        dec = jnp.zeros((8, LANES), F32)
        before = jnp.zeros((8, LANES), F32)
        for c in range(segs):
            rows = slice(c * SEG, (c + 1) * SEG)
            cum = jnp.dot(tri, logs[rows], precision=lax.Precision.HIGHEST, preferred_element_type=F32)
            last = cum[SEG - 1:SEG]
            wst[rows, :] = jnp.exp(last - cum) * dt[rows]
            gl_ref[rows, :] = cum * LOG2E
            qt_ref[rows, :] = jnp.transpose(cum * LOG2E - jnp.log2(dt[rows]))
            bt_ref[rows, :] = jnp.transpose(bc[rows, :STATE].astype(F32)).astype(BF16)
            dec = jnp.where(row == c, jnp.exp(last), dec)
            before = jnp.where(row == c, jnp.exp(total), before)
            total = total + last
        seg_dec[...] = dec
        dec_ref[...] = before
        lsend[...] = jnp.broadcast_to(total, (8, LANES))

    def s_of(mine, c):
        return jnp.where(mine, s_own[c, core], rc[c])

    @pl.when(step == 1)
    def _():
        pl.semaphore_wait(barrier, 7)
        for store in stores:
            store.start()
        for k in range(1, 8):
            log_copy(k).start()
        lall[me] = lsend[...]

    @pl.when(at_lag(2))
    def _():
        core_copy(step - 2).start()

    @pl.when(step == 2)
    def _():
        for k in range(1, 8):
            log_copy(k).wait_send()
            source = other(k)
            pltpu.make_async_remote_copy(
                src_ref=lsend, dst_ref=lall.at[source], send_sem=lsem.at[k - 1], recv_sem=lrem.at[source],
                device_id={"sp": source}, device_id_type=MESH).wait_recv()
        chip = ypos * 4
        row = lax.broadcasted_iota(jnp.int32, (8, LANES), 0)
        logs = jnp.where(row == 0, lall[me - core + 1], 0.0)
        logs = jnp.where(row == 1, lall[chip + 2] + lall[chip + 3], logs)
        logs = jnp.where(jnp.logical_and(row == 2, xpos == 1), lall[chip] + lall[chip + 1], logs)
        logs = jnp.where(row == 3, lall[me - core], logs)
        decays = jnp.exp(logs)
        for c in range(tiles):
            drow[c] = spread(lane_shift(decays, c * TILE_HEADS + core * (TILE_HEADS // 2)), 2)

    @pl.when(at_lag(3))
    def _():
        c = step - 3
        core_copy(c).wait()
        sx[c] = drow[c, 0:1] * s_of(core == 0, c) + s_of(core == 1, c)

    @pl.when(at_lag(4))
    def _():
        x_copy(step - 4).start()

    @pl.when(at_lag(LAG_X))
    def _():
        c = step - LAG_X
        x_copy(c).wait()
        mine, got = sx[c], rx[c]
        early = jnp.where(xpos == 0, mine, got)
        late = jnp.where(xpos == 0, got, mine)
        sy[c] = drow[c, 1:2] * early + late

    @pl.when(at_lag(LAG_X + 1))
    def _():
        y_copy(step - LAG_X - 1).start()

    @pl.when(at_lag(LAG_Y))
    def _():
        c = step - LAG_Y
        y_copy(c).wait()
        before = jnp.where(xpos == 1, rx[c], 0.0) + jnp.where(ypos == 1, drow[c, 2:3] * ry[c], 0.0)
        after = drow[c, 3:4] * before + s_of(core == 0, c)
        sx[c] = jnp.where(core == 0, before, after)
        sy[c] = jnp.where(core == 0, after, before)

    @pl.when(at_lag(LAG_Y + 1))
    def _():
        final_copy(step - LAG_Y - 1).start()

    @pl.when(at_lag(LAG_Y + 2))
    def _():
        c = step - LAG_Y - 2
        final_copy(c).wait()
        mine, got = sx[c], rf[c]
        hin_ref[:, :HALF] = jnp.where(core == 0, mine, got)
        hin_ref[:, HALF:] = jnp.where(core == 0, got, mine)

    with_state = jnp.logical_and(step >= 1, step <= tiles)

    @pl.when(with_state)
    def _():
        weigh(step - 1)
        project_half(0)
        states(step - 1)
        project_half(1)

    @pl.when(jnp.logical_not(with_state))
    def _():
        for h in range(2):
            project_half(h)

    @pl.when(step == 2 * tiles - 1)
    def _():
        for store in stores:
            store.wait()


def mix_kernel(z_ref, xs_ref, loc_ref, h_ref, bc_ref, gl_ref, qt_ref, dec_ref, ds_ref, w_hbm, x_hbm,
               out_hbm, acc, gated_a, gated_b, scores, wbuf, out_ref, w_sem, x_sem, o_sem):
    step = pl.program_id(0)
    steps = pl.num_programs(0)
    tokens, d_model = acc.shape
    segs = tokens // SEG
    slots = wbuf.shape[0]
    groups = w_hbm.shape[0] // TILE
    x_copy = pltpu.make_async_copy(x_hbm, out_ref, x_sem)

    def w_copy(group):
        slot = lax.rem(group, slots)
        first = pl.multiple_of(group * TILE, TILE)
        return pltpu.make_async_copy(w_hbm.at[pl.ds(first, TILE), :], wbuf.at[slot], w_sem.at[slot])

    def w_next(group):
        @pl.when(group + slots < groups)
        def _():
            w_copy(group + slots).start()

    def dot_slice(k, source, group):
        cols = slice(k * TILE, (k + 1) * TILE)
        acc[:, cols] += dot32(source[...], wbuf[lax.rem(group, slots), :, cols])

    def group_outputs(half, target, big):
        base = half * TILE
        first = (2 * step + half) * TILE_HEADS
        gl = lane_shift(gl_ref[...], first)
        dec = spread(lane_shift(dec_ref[...], first), TILE_HEADS // 2)
        skip = spread(lane_shift(jnp.broadcast_to(ds_ref[...], (8, LANES)), first), TILE_HEADS // 2)[:1]
        causal = (lax.broadcasted_iota(jnp.int32, (SEG, SEG), 0)
                  >= lax.broadcasted_iota(jnp.int32, (SEG, SEG), 1))
        low = lax.broadcasted_iota(jnp.int32, (SEG, LANES), 1) < HEAD_DIM
        zero = jnp.zeros((SEG, LANES), BF16)
        pending = None
        unit = 0
        for c in range(segs):
            rows = slice(c * SEG, (c + 1) * SEG)
            state = h_ref[:, base:base + TILE]
            if c > 0:
                state = dec[c:c + 1] * state + loc_ref[(c - 1) * STATE:c * STATE, base:base + TILE]
            y_state = dot32(bc_ref[rows, STATE:], state.astype(BF16))
            q_rows = qt_ref[pl.ds(pl.multiple_of(c * SEG + first, TILE_HEADS), TILE_HEADS), :]
            for p in range(TILE_HEADS // 2):
                cols = slice(base + p * LANES, base + (p + 1) * LANES)
                sc = scores[rows, :]
                col_a = jnp.broadcast_to(gl[rows, 2 * p:2 * p + 1], (SEG, LANES))
                col_b = jnp.broadcast_to(gl[rows, 2 * p + 1:2 * p + 2], (SEG, LANES))
                g_a = jnp.where(causal, sc * jnp.exp2(col_a - q_rows[2 * p:2 * p + 1]), 0.0).astype(BF16)
                g_b = jnp.where(causal, sc * jnp.exp2(col_b - q_rows[2 * p + 1:2 * p + 2]), 0.0).astype(BF16)
                xp = xs_ref[rows, cols]
                rhs = jnp.concatenate([jnp.where(low, xp, zero), jnp.where(low, zero, xp)], axis=0)
                if unit % 2 == 0 and big is not None:
                    dot_slice(unit // 2, *big)
                y = dot32(jnp.concatenate([g_a, g_b], axis=1), rhs)
                if pending is not None:
                    pending()

                def pending(y=y, rows=rows, cols=cols, p=p, y_state=y_state, col_a=col_a, col_b=col_b):
                    here = slice(p * LANES, (p + 1) * LANES)
                    total = y + y_state[:, here] * jnp.exp2(jnp.where(low, col_a, col_b))
                    total = total + skip[:, here] * xs_ref[rows, cols].astype(F32)
                    z = z_ref[rows, cols].astype(F32)
                    target[rows, here] = (total * (z / (1.0 + jnp.exp(-z)))).astype(BF16)
                unit += 1
        pending()

    @pl.when(step == 0)
    def _():
        for group in range(slots):
            w_copy(group).start()
        x_copy.start()
        acc[...] = jnp.zeros_like(acc)
        for c in range(segs):
            rows = slice(c * SEG, (c + 1) * SEG)
            scores[rows, :] = lax.dot_general(bc_ref[rows, STATE:], bc_ref[rows, :STATE],
                                              (((1,), (1,)), ((), ())), preferred_element_type=F32)
        group_outputs(0, gated_a, None)

    @pl.when(jnp.logical_and(step > 0, step < steps - 1))
    def _():
        w_copy(2 * step - 1).wait()
        group_outputs(0, gated_a, (gated_b, 2 * step - 1))
        w_next(2 * step - 1)

    @pl.when(step < steps - 1)
    def _():
        w_copy(2 * step).wait()
        group_outputs(1, gated_b, (gated_a, 2 * step))
        w_next(2 * step)

    @pl.when(step == steps - 1)
    def _():
        x_copy.wait()
        w_copy(groups - 1).wait()
        copies = []
        for k in range(d_model // (2 * TILE)):
            cols = slice(2 * k * TILE, 2 * (k + 1) * TILE)
            total = acc[:, cols] + dot32(gated_b[...], wbuf[(groups - 1) % slots, :, cols])
            out_ref[:, cols] = (out_ref[:, cols].astype(F32) + total).astype(BF16)
            copies.append(pltpu.make_async_copy(out_ref.at[:, cols], out_hbm.at[:, cols], o_sem.at[k]))
            copies[-1].start()
        for copy in copies:
            copy.wait()


def solution(mesh):
    row_spec = P(("dp", "sp"), None)

    def local_mixer(x_loc, w_in, a_neg, dt_bias, d_skip, w_out):
        tokens, d_model = x_loc.shape
        inner = w_out.shape[0]
        heads = a_neg.shape[0]
        tiles = inner // TILE
        segs = tokens // SEG
        assert mesh.shape["sp"] == 8 and heads == LANES and inner == heads * HEAD_DIM
        assert tiles >= LAG_Y + 2
        def fixed(shape):
            return pl.BlockSpec(shape, lambda i: (0,) * len(shape), pipeline_mode=pl.Buffered(1))

        half = (tiles, STATE, HALF)
        sems = pltpu.SemaphoreType.DMA((tiles,))
        any_space = pl.BlockSpec(memory_space=pl.ANY)
        u, loc, h_in, bc, gl, qt, dec = pl.pallas_call(
            project_kernel,
            grid=(2 * tiles,),
            out_shape=[
                jax.ShapeDtypeStruct((tokens, 2 * inner), BF16),
                jax.ShapeDtypeStruct(((segs - 1) * STATE, inner), F32),
                jax.ShapeDtypeStruct((STATE, inner), F32),
                jax.ShapeDtypeStruct((tokens, 2 * STATE), BF16),
                jax.ShapeDtypeStruct((tokens, heads), F32),
                jax.ShapeDtypeStruct((segs * heads, SEG), F32),
                jax.ShapeDtypeStruct((8, heads), F32),
            ],
            in_specs=[
                any_space,
                pl.BlockSpec((d_model, TILE), lambda i: (0, lax.rem(i + tiles, 2 * tiles))),
                any_space, any_space, any_space,
            ],
            out_specs=[
                pl.BlockSpec((tokens, TILE), lambda i: (0, lax.rem(i + tiles, 2 * tiles))),
                pl.BlockSpec(((segs - 1) * STATE, TILE), lambda i: (0, jnp.clip(i - 1, 0, tiles - 1))),
                pl.BlockSpec((STATE, TILE), lambda i: (0, jnp.maximum(i - (LAG_Y + 2), 0))),
                any_space, any_space, any_space, any_space,
            ],
            scratch_shapes=[
                pltpu.VMEM((tokens, d_model), BF16),
                pltpu.VMEM((d_model, 2 * STATE), BF16),
                pltpu.VMEM((d_model, heads), BF16),
                pltpu.VMEM((1, heads), F32), pltpu.VMEM((1, heads), F32),
                pltpu.VMEM((tokens, 2 * STATE), BF16),
                pltpu.VMEM((tokens, heads), F32),
                pltpu.VMEM((segs * heads, SEG), F32),
                pltpu.VMEM((8, heads), F32),
                pltpu.SemaphoreType.DMA((5,)), pltpu.SemaphoreType.DMA((4,)),
                pltpu.VMEM((segs * STATE, SEG), BF16),
                pltpu.VMEM((8, heads), F32),
                pltpu.VMEM((tokens, TILE), BF16),
                pltpu.VMEM((tokens, heads), F32),
                pltpu.VMEM((tokens, TILE), BF16),
                pltpu.VMEM((tiles, 8, HALF), F32),
                pltpu.VMEM((8, heads), F32),
                pltpu.VMEM((8, 8, heads), F32),
                pltpu.VMEM((tiles, 2, STATE, HALF), F32),
                pltpu.VMEM(half, F32), pltpu.VMEM(half, F32), pltpu.VMEM(half, F32),
                pltpu.VMEM(half, F32), pltpu.VMEM(half, F32), pltpu.VMEM(half, F32),
                pltpu.SemaphoreType.DMA((7,)), pltpu.SemaphoreType.DMA((8,)),
                sems, sems, sems, sems, sems, sems, sems, sems,
            ],
            compiler_params=pltpu.CompilerParams(
                dimension_semantics=("arbitrary",), collective_id=0, has_side_effects=True,
                vmem_limit_bytes=60 * 1024 * 1024),
            cost_estimate=pl.CostEstimate(flops=2 * tokens * d_model * w_in.shape[1],
                                          bytes_accessed=2 * w_in.size, transcendentals=0),
            name="project",
        )(x_loc, w_in, w_in, a_neg.reshape(1, heads), dt_bias.reshape(1, heads))

        last = tiles // 2 - 1
        return pl.pallas_call(
            mix_kernel,
            grid=(tiles // 2 + 1,),
            out_shape=jax.ShapeDtypeStruct((tokens, d_model), BF16),
            in_specs=[
                pl.BlockSpec((tokens, 2 * TILE), lambda i: (0, jnp.minimum(i, last))),
                pl.BlockSpec((tokens, 2 * TILE), lambda i: (0, jnp.minimum(i, last) + tiles // 2)),
                pl.BlockSpec(((segs - 1) * STATE, 2 * TILE), lambda i: (0, jnp.minimum(i, last))),
                pl.BlockSpec((STATE, 2 * TILE), lambda i: (0, jnp.minimum(i, last))),
                fixed((tokens, 2 * STATE)), fixed((tokens, heads)),
                fixed((segs * heads, SEG)), fixed((8, heads)), fixed((1, heads)),
                any_space, any_space,
            ],
            out_specs=any_space,
            scratch_shapes=[
                pltpu.VMEM((tokens, d_model), F32),
                pltpu.VMEM((tokens, TILE), BF16),
                pltpu.VMEM((tokens, TILE), BF16),
                pltpu.VMEM((tokens, SEG), F32),
                pltpu.VMEM((4, TILE, d_model), BF16),
                pltpu.VMEM((tokens, d_model), BF16),
                pltpu.SemaphoreType.DMA((4,)),
                pltpu.SemaphoreType.DMA(()),
                pltpu.SemaphoreType.DMA((d_model // (2 * TILE),)),
            ],
            compiler_params=pltpu.CompilerParams(
                dimension_semantics=("arbitrary",), vmem_limit_bytes=62 * 1024 * 1024),
            cost_estimate=pl.CostEstimate(flops=2 * tokens * d_model * inner,
                                          bytes_accessed=2 * w_out.size, transcendentals=0),
            name="mix",
        )(u, u, loc, h_in, bc, gl, qt, dec, d_skip.reshape(1, heads), w_out, x_loc)

    return jax.shard_map(local_mixer, mesh=mesh, in_specs=(row_spec, P(), P(), P(), P(), P()),
                         out_specs=row_spec, check_vma=False)
```

```python
import jax
import jax.numpy as jnp
from jax import lax
from jax.experimental import pallas as pl
from jax.experimental.pallas import tpu as pltpu
from jax.sharding import PartitionSpec as P

SEG = 128
HEAD_DIM = 64
STATE = 128
TILE = 512
HALF = TILE // 2
TILE_HEADS = TILE // HEAD_DIM
LANES = 128
LAG_X = 9
LAG_Y = 14
LOG2E = 1.4426950408889634
MESH = pl.DeviceIdType.MESH
BF16 = jnp.bfloat16
F32 = jnp.float32


def dot32(a, b):
    return jnp.dot(a, b, preferred_element_type=F32)


def spread(v, pairs):
    rows = v.shape[0]
    low = lax.broadcasted_iota(jnp.int32, (rows, LANES), 1) < HEAD_DIM
    parts = []
    for p in range(pairs):
        left = jnp.broadcast_to(v[:, 2 * p:2 * p + 1], (rows, LANES))
        right = jnp.broadcast_to(v[:, 2 * p + 1:2 * p + 2], (rows, LANES))
        parts.append(jnp.where(low, left, right))
    return jnp.concatenate(parts, axis=1)


def lane_shift(v, first):
    return pltpu.roll(v, lax.rem(LANES - first, LANES), 1)


def project_kernel(x_hbm, w_ref, w_hbm, an_hbm, db_hbm,
                   u_ref, loc_ref, hin_ref, bc_hbm, gl_hbm, qt_hbm, dec_hbm,
                   x_ref, wdt_ref, an_ref, db_ref, bc_ref, gl_ref, qt_ref, dec_ref, isem, osem,
                   bt_ref, seg_dec, xw_ref, wst, uprev, drow, lsend, lall, s_own, rc, sx, rx, sy, ry, rf,
                   lsem, lrem, csem, crem, xsem, xrem, ysem, yrem, fsem, frem):
    step = pl.program_id(0)
    me = lax.axis_index("sp")
    tokens = x_ref.shape[0]
    segs = tokens // SEG
    tiles = s_own.shape[0]
    heads_at = 2 * tiles * TILE
    loads = [
        pltpu.make_async_copy(db_hbm, db_ref, isem.at[0]),
        pltpu.make_async_copy(an_hbm, an_ref, isem.at[1]),
        pltpu.make_async_copy(x_hbm, x_ref, isem.at[2]),
        pltpu.make_async_copy(w_hbm.at[:, heads_at:], wdt_ref, isem.at[3]),
    ]
    stores = [
        pltpu.make_async_copy(bc_ref, bc_hbm, osem.at[0]),
        pltpu.make_async_copy(gl_ref, gl_hbm, osem.at[1]),
        pltpu.make_async_copy(qt_ref, qt_hbm, osem.at[2]),
        pltpu.make_async_copy(dec_ref, dec_hbm, osem.at[3]),
    ]
    core = lax.rem(me, 2)
    xpos = lax.rem(me // 2, 2)
    ypos = me // 4
    peer_core = me + 1 - 2 * core
    peer_x = me + 2 - 4 * xpos
    peer_y = me + 4 - 8 * ypos
    barrier = pltpu.get_barrier_semaphore()

    def other(k):
        return lax.rem(me + k, 8)

    def log_copy(k):
        return pltpu.make_async_remote_copy(
            src_ref=lsend, dst_ref=lall.at[me], send_sem=lsem.at[k - 1], recv_sem=lrem.at[me],
            device_id={"sp": other(k)}, device_id_type=MESH)

    def remote(src, dst, send, recv, target):
        return pltpu.make_async_remote_copy(
            src_ref=src, dst_ref=dst, send_sem=send, recv_sem=recv,
            device_id={"sp": target}, device_id_type=MESH)

    def core_copy(c):
        return remote(s_own.at[c, 1 - core], rc.at[c], csem.at[c], crem.at[c], peer_core)

    def x_copy(c):
        return remote(sx.at[c], rx.at[c], xsem.at[c], xrem.at[c], peer_x)

    def y_copy(c):
        return remote(sy.at[c], ry.at[c], ysem.at[c], yrem.at[c], peer_y)

    def final_copy(c):
        return remote(sy.at[c], rf.at[c], fsem.at[c], frem.at[c], peer_core)

    def at_lag(lag):
        return jnp.logical_and(step >= lag, step < tiles + lag)

    def weigh(tile):
        weights = lane_shift(wst[...], tile * TILE_HEADS)
        for c in range(segs):
            rows = slice(c * SEG, (c + 1) * SEG)
            spread_rows = spread(weights[rows], TILE_HEADS // 2)
            xw_ref[rows, :] = (uprev[rows, :].astype(F32) * spread_rows).astype(BF16)

    def states(tile):
        dec = spread(lane_shift(seg_dec[...], tile * TILE_HEADS), TILE_HEADS // 2)
        state = dot32(bt_ref[:SEG, :], xw_ref[:SEG, :])
        for c in range(1, segs):
            rows = slice(c * SEG, (c + 1) * SEG)
            loc_ref[(c - 1) * STATE:c * STATE, :] = state
            state = dec[c:c + 1] * state + dot32(bt_ref[rows, :], xw_ref[rows, :])
        s_own[tile, 0] = state[:, :HALF]
        s_own[tile, 1] = state[:, HALF:]

    def project():
        u = dot32(x_ref[...], w_ref[...]).astype(BF16)
        u_ref[...] = u
        uprev[...] = u

    @pl.when(step == 0)
    def _():
        for k in range(1, 8):
            pl.semaphore_signal(barrier, inc=1, device_id={"sp": other(k)}, device_id_type=MESH)
        for load in loads:
            load.start()
        for load in loads:
            load.wait()
        last_columns = dot32(x_ref[...], wdt_ref[...]).astype(BF16)
        bc = last_columns[:, :2 * STATE]
        bc_ref[...] = bc
        raw = last_columns[:, 2 * STATE:].astype(F32) + db_ref[...]
        dt = jnp.maximum(raw, 0.0) + jnp.log1p(jnp.exp(-jnp.abs(raw)))
        logs = dt * an_ref[...]
        tri = (lax.broadcasted_iota(jnp.int32, (SEG, SEG), 0)
               >= lax.broadcasted_iota(jnp.int32, (SEG, SEG), 1)).astype(F32)
        total = jnp.zeros((1, LANES), F32)
        row = lax.broadcasted_iota(jnp.int32, (8, LANES), 0)
        dec = jnp.zeros((8, LANES), F32)
        before = jnp.zeros((8, LANES), F32)
        for c in range(segs):
            rows = slice(c * SEG, (c + 1) * SEG)
            cum = jnp.dot(tri, logs[rows], precision=lax.Precision.HIGHEST, preferred_element_type=F32)
            last = cum[SEG - 1:SEG]
            wst[rows, :] = jnp.exp(last - cum) * dt[rows]
            gl_ref[rows, :] = cum * LOG2E
            qt_ref[rows, :] = jnp.transpose(cum * LOG2E - jnp.log2(dt[rows]))
            bt_ref[rows, :] = jnp.transpose(bc[rows, :STATE].astype(F32)).astype(BF16)
            dec = jnp.where(row == c, jnp.exp(last), dec)
            before = jnp.where(row == c, jnp.exp(total), before)
            total = total + last
        seg_dec[...] = dec
        dec_ref[...] = before
        lsend[...] = jnp.broadcast_to(total, (8, LANES))

    def s_of(mine, c):
        return jnp.where(mine, s_own[c, core], rc[c])

    @pl.when(step == 1)
    def _():
        pl.semaphore_wait(barrier, 7)
        for store in stores:
            store.start()
        for k in range(1, 8):
            log_copy(k).start()
        lall[me] = lsend[...]

    @pl.when(at_lag(3))
    def _():
        core_copy(step - 3).start()

    @pl.when(step == 2)
    def _():
        for k in range(1, 8):
            log_copy(k).wait_send()
            source = other(k)
            pltpu.make_async_remote_copy(
                src_ref=lsend, dst_ref=lall.at[source], send_sem=lsem.at[k - 1], recv_sem=lrem.at[source],
                device_id={"sp": source}, device_id_type=MESH).wait_recv()
        chip = ypos * 4
        row = lax.broadcasted_iota(jnp.int32, (8, LANES), 0)
        logs = jnp.where(row == 0, lall[me - core + 1], 0.0)
        logs = jnp.where(row == 1, lall[chip + 2] + lall[chip + 3], logs)
        logs = jnp.where(jnp.logical_and(row == 2, xpos == 1), lall[chip] + lall[chip + 1], logs)
        logs = jnp.where(row == 3, lall[me - core], logs)
        decays = jnp.exp(logs)
        for c in range(tiles):
            drow[c] = spread(lane_shift(decays, c * TILE_HEADS + core * (TILE_HEADS // 2)), 2)

    @pl.when(at_lag(4))
    def _():
        c = step - 4
        core_copy(c).wait()
        sx[c] = drow[c, 0:1] * s_of(core == 0, c) + s_of(core == 1, c)

    @pl.when(at_lag(5))
    def _():
        x_copy(step - 5).start()

    @pl.when(at_lag(LAG_X))
    def _():
        c = step - LAG_X
        x_copy(c).wait()
        mine, got = sx[c], rx[c]
        early = jnp.where(xpos == 0, mine, got)
        late = jnp.where(xpos == 0, got, mine)
        sy[c] = drow[c, 1:2] * early + late

    @pl.when(at_lag(LAG_X + 1))
    def _():
        y_copy(step - LAG_X - 1).start()

    @pl.when(at_lag(LAG_Y))
    def _():
        c = step - LAG_Y
        y_copy(c).wait()
        before = jnp.where(xpos == 1, rx[c], 0.0) + jnp.where(ypos == 1, drow[c, 2:3] * ry[c], 0.0)
        after = drow[c, 3:4] * before + s_of(core == 0, c)
        sx[c] = jnp.where(core == 0, before, after)
        sy[c] = jnp.where(core == 0, after, before)

    @pl.when(at_lag(LAG_Y + 1))
    def _():
        final_copy(step - LAG_Y - 1).start()

    @pl.when(at_lag(LAG_Y + 2))
    def _():
        c = step - LAG_Y - 2
        final_copy(c).wait()
        mine, got = sx[c], rf[c]
        hin_ref[:, :HALF] = jnp.where(core == 0, mine, got)
        hin_ref[:, HALF:] = jnp.where(core == 0, got, mine)

    with_state = jnp.logical_and(step >= 1, step <= tiles + 1)

    @pl.when(with_state)
    def _():
        states(jnp.maximum(step - 2, 0))
        weigh(step - 1)
        project()

    @pl.when(jnp.logical_not(with_state))
    def _():
        project()

    @pl.when(step == 2 * tiles - 1)
    def _():
        for store in stores:
            store.wait()


def mix_kernel(z_ref, xs_ref, loc_ref, h_ref, bc_ref, gl_ref, qt_ref, dec_ref, ds_ref, w_hbm, x_hbm,
               out_hbm, acc, gated_a, gated_b, scores, wbuf, out_ref, w_sem, x_sem, o_sem):
    step = pl.program_id(0)
    steps = pl.num_programs(0)
    tokens, d_model = acc.shape
    segs = tokens // SEG
    slots = wbuf.shape[0]
    groups = w_hbm.shape[0] // TILE
    x_copy = pltpu.make_async_copy(x_hbm, out_ref, x_sem)

    def w_copy(group):
        slot = lax.rem(group, slots)
        first = pl.multiple_of(group * TILE, TILE)
        return pltpu.make_async_copy(w_hbm.at[pl.ds(first, TILE), :], wbuf.at[slot], w_sem.at[slot])

    def w_next(group):
        @pl.when(group + slots < groups)
        def _():
            w_copy(group + slots).start()

    def dot_slice(k, source, group):
        cols = slice(k * TILE, (k + 1) * TILE)
        acc[:, cols] += dot32(source[...], wbuf[lax.rem(group, slots), :, cols])

    def group_outputs(half, target, big):
        base = half * TILE
        first = (2 * step + half) * TILE_HEADS
        gl = lane_shift(gl_ref[...], first)
        dec = spread(lane_shift(dec_ref[...], first), TILE_HEADS // 2)
        skip = spread(lane_shift(jnp.broadcast_to(ds_ref[...], (8, LANES)), first), TILE_HEADS // 2)[:1]
        causal = (lax.broadcasted_iota(jnp.int32, (SEG, SEG), 0)
                  >= lax.broadcasted_iota(jnp.int32, (SEG, SEG), 1))
        low = lax.broadcasted_iota(jnp.int32, (SEG, LANES), 1) < HEAD_DIM
        zero = jnp.zeros((SEG, LANES), BF16)
        pending = None
        unit = 0
        for c in range(segs):
            rows = slice(c * SEG, (c + 1) * SEG)
            state = h_ref[:, base:base + TILE]
            if c > 0:
                state = dec[c:c + 1] * state + loc_ref[(c - 1) * STATE:c * STATE, base:base + TILE]
            y_state = dot32(bc_ref[rows, STATE:], state.astype(BF16))
            q_rows = qt_ref[pl.ds(pl.multiple_of(c * SEG + first, TILE_HEADS), TILE_HEADS), :]
            for p in range(TILE_HEADS // 2):
                cols = slice(base + p * LANES, base + (p + 1) * LANES)
                sc = scores[rows, :]
                col_a = jnp.broadcast_to(gl[rows, 2 * p:2 * p + 1], (SEG, LANES))
                col_b = jnp.broadcast_to(gl[rows, 2 * p + 1:2 * p + 2], (SEG, LANES))
                g_a = jnp.where(causal, sc * jnp.exp2(col_a - q_rows[2 * p:2 * p + 1]), 0.0).astype(BF16)
                g_b = jnp.where(causal, sc * jnp.exp2(col_b - q_rows[2 * p + 1:2 * p + 2]), 0.0).astype(BF16)
                xp = xs_ref[rows, cols]
                rhs = jnp.concatenate([jnp.where(low, xp, zero), jnp.where(low, zero, xp)], axis=0)
                if unit % 2 == 0 and big is not None:
                    dot_slice(unit // 2, *big)
                y = dot32(jnp.concatenate([g_a, g_b], axis=1), rhs)
                if pending is not None:
                    pending()

                def pending(y=y, rows=rows, cols=cols, p=p, y_state=y_state, col_a=col_a, col_b=col_b):
                    here = slice(p * LANES, (p + 1) * LANES)
                    total = y + y_state[:, here] * jnp.exp2(jnp.where(low, col_a, col_b))
                    total = total + skip[:, here] * xs_ref[rows, cols].astype(F32)
                    z = z_ref[rows, cols].astype(F32)
                    target[rows, here] = (total * (z / (1.0 + jnp.exp(-z)))).astype(BF16)
                unit += 1
        pending()

    @pl.when(step == 0)
    def _():
        for group in range(slots):
            w_copy(group).start()
        x_copy.start()
        acc[...] = jnp.zeros_like(acc)
        for c in range(segs):
            rows = slice(c * SEG, (c + 1) * SEG)
            scores[rows, :] = lax.dot_general(bc_ref[rows, STATE:], bc_ref[rows, :STATE],
                                              (((1,), (1,)), ((), ())), preferred_element_type=F32)
        group_outputs(0, gated_a, None)

    @pl.when(jnp.logical_and(step > 0, step < steps - 1))
    def _():
        w_copy(2 * step - 1).wait()
        group_outputs(0, gated_a, (gated_b, 2 * step - 1))
        w_next(2 * step - 1)

    @pl.when(step < steps - 1)
    def _():
        w_copy(2 * step).wait()
        group_outputs(1, gated_b, (gated_a, 2 * step))
        w_next(2 * step)

    @pl.when(step == steps - 1)
    def _():
        x_copy.wait()
        w_copy(groups - 1).wait()
        copies = []
        for k in range(d_model // (2 * TILE)):
            cols = slice(2 * k * TILE, 2 * (k + 1) * TILE)
            total = acc[:, cols] + dot32(gated_b[...], wbuf[(groups - 1) % slots, :, cols])
            out_ref[:, cols] = (out_ref[:, cols].astype(F32) + total).astype(BF16)
            copies.append(pltpu.make_async_copy(out_ref.at[:, cols], out_hbm.at[:, cols], o_sem.at[k]))
            copies[-1].start()
        for copy in copies:
            copy.wait()


def solution(mesh):
    row_spec = P(("dp", "sp"), None)

    def local_mixer(x_loc, w_in, a_neg, dt_bias, d_skip, w_out):
        tokens, d_model = x_loc.shape
        inner = w_out.shape[0]
        heads = a_neg.shape[0]
        tiles = inner // TILE
        segs = tokens // SEG
        assert mesh.shape["sp"] == 8 and heads == LANES and inner == heads * HEAD_DIM
        assert tiles >= LAG_Y + 2
        def fixed(shape):
            return pl.BlockSpec(shape, lambda i: (0,) * len(shape), pipeline_mode=pl.Buffered(1))

        half = (tiles, STATE, HALF)
        sems = pltpu.SemaphoreType.DMA((tiles,))
        any_space = pl.BlockSpec(memory_space=pl.ANY)
        u, loc, h_in, bc, gl, qt, dec = pl.pallas_call(
            project_kernel,
            grid=(2 * tiles,),
            out_shape=[
                jax.ShapeDtypeStruct((tokens, 2 * inner), BF16),
                jax.ShapeDtypeStruct(((segs - 1) * STATE, inner), F32),
                jax.ShapeDtypeStruct((STATE, inner), F32),
                jax.ShapeDtypeStruct((tokens, 2 * STATE), BF16),
                jax.ShapeDtypeStruct((tokens, heads), F32),
                jax.ShapeDtypeStruct((segs * heads, SEG), F32),
                jax.ShapeDtypeStruct((8, heads), F32),
            ],
            in_specs=[
                any_space,
                pl.BlockSpec((d_model, TILE), lambda i: (0, lax.rem(i + tiles, 2 * tiles))),
                any_space, any_space, any_space,
            ],
            out_specs=[
                pl.BlockSpec((tokens, TILE), lambda i: (0, lax.rem(i + tiles, 2 * tiles))),
                pl.BlockSpec(((segs - 1) * STATE, TILE), lambda i: (0, jnp.clip(i - 2, 0, tiles - 1))),
                pl.BlockSpec((STATE, TILE), lambda i: (0, jnp.maximum(i - (LAG_Y + 2), 0))),
                any_space, any_space, any_space, any_space,
            ],
            scratch_shapes=[
                pltpu.VMEM((tokens, d_model), BF16),
                pltpu.VMEM((d_model, 2 * STATE + heads), BF16),
                pltpu.VMEM((1, heads), F32), pltpu.VMEM((1, heads), F32),
                pltpu.VMEM((tokens, 2 * STATE), BF16),
                pltpu.VMEM((tokens, heads), F32),
                pltpu.VMEM((segs * heads, SEG), F32),
                pltpu.VMEM((8, heads), F32),
                pltpu.SemaphoreType.DMA((4,)), pltpu.SemaphoreType.DMA((4,)),
                pltpu.VMEM((segs * STATE, SEG), BF16),
                pltpu.VMEM((8, heads), F32),
                pltpu.VMEM((tokens, TILE), BF16),
                pltpu.VMEM((tokens, heads), F32),
                pltpu.VMEM((tokens, TILE), BF16),
                pltpu.VMEM((tiles, 8, HALF), F32),
                pltpu.VMEM((8, heads), F32),
                pltpu.VMEM((8, 8, heads), F32),
                pltpu.VMEM((tiles, 2, STATE, HALF), F32),
                pltpu.VMEM(half, F32), pltpu.VMEM(half, F32), pltpu.VMEM(half, F32),
                pltpu.VMEM(half, F32), pltpu.VMEM(half, F32), pltpu.VMEM(half, F32),
                pltpu.SemaphoreType.DMA((7,)), pltpu.SemaphoreType.DMA((8,)),
                sems, sems, sems, sems, sems, sems, sems, sems,
            ],
            compiler_params=pltpu.CompilerParams(
                dimension_semantics=("arbitrary",), collective_id=0, has_side_effects=True,
                vmem_limit_bytes=60 * 1024 * 1024),
            cost_estimate=pl.CostEstimate(flops=2 * tokens * d_model * w_in.shape[1],
                                          bytes_accessed=2 * w_in.size, transcendentals=0),
            name="project",
        )(x_loc, w_in, w_in, a_neg.reshape(1, heads), dt_bias.reshape(1, heads))

        last = tiles // 2 - 1
        return pl.pallas_call(
            mix_kernel,
            grid=(tiles // 2 + 1,),
            out_shape=jax.ShapeDtypeStruct((tokens, d_model), BF16),
            in_specs=[
                pl.BlockSpec((tokens, 2 * TILE), lambda i: (0, jnp.minimum(i, last))),
                pl.BlockSpec((tokens, 2 * TILE), lambda i: (0, jnp.minimum(i, last) + tiles // 2)),
                pl.BlockSpec(((segs - 1) * STATE, 2 * TILE), lambda i: (0, jnp.minimum(i, last))),
                pl.BlockSpec((STATE, 2 * TILE), lambda i: (0, jnp.minimum(i, last))),
                fixed((tokens, 2 * STATE)), fixed((tokens, heads)),
                fixed((segs * heads, SEG)), fixed((8, heads)), fixed((1, heads)),
                any_space, any_space,
            ],
            out_specs=any_space,
            scratch_shapes=[
                pltpu.VMEM((tokens, d_model), F32),
                pltpu.VMEM((tokens, TILE), BF16),
                pltpu.VMEM((tokens, TILE), BF16),
                pltpu.VMEM((tokens, SEG), F32),
                pltpu.VMEM((4, TILE, d_model), BF16),
                pltpu.VMEM((tokens, d_model), BF16),
                pltpu.SemaphoreType.DMA((4,)),
                pltpu.SemaphoreType.DMA(()),
                pltpu.SemaphoreType.DMA((d_model // (2 * TILE),)),
            ],
            compiler_params=pltpu.CompilerParams(
                dimension_semantics=("arbitrary",), vmem_limit_bytes=62 * 1024 * 1024),
            cost_estimate=pl.CostEstimate(flops=2 * tokens * d_model * inner,
                                          bytes_accessed=2 * w_out.size, transcendentals=0),
            name="mix",
        )(u, u, loc, h_in, bc, gl, qt, dec, d_skip.reshape(1, heads), w_out, x_loc)

    return jax.shard_map(local_mixer, mesh=mesh, in_specs=(row_spec, P(), P(), P(), P(), P()),
                         out_specs=row_spec, check_vma=False)
```

```python
import jax
import jax.numpy as jnp
from jax import lax
from jax.experimental import pallas as pl
from jax.experimental.pallas import tpu as pltpu
from jax.sharding import PartitionSpec as P

SEG = 128
HEAD_DIM = 64
STATE = 128
TILE = 512
HALF = TILE // 2
TILE_HEADS = TILE // HEAD_DIM
LANES = 128
CHUNKS = 4
LAG_X = 9
LAG_Y = 14
LOG2E = 1.4426950408889634
MESH = pl.DeviceIdType.MESH
BF16 = jnp.bfloat16
F32 = jnp.float32


def dot32(a, b):
    return jnp.dot(a, b, preferred_element_type=F32)


def spread(v, pairs):
    rows = v.shape[0]
    low = lax.broadcasted_iota(jnp.int32, (rows, LANES), 1) < HEAD_DIM
    parts = []
    for p in range(pairs):
        left = jnp.broadcast_to(v[:, 2 * p:2 * p + 1], (rows, LANES))
        right = jnp.broadcast_to(v[:, 2 * p + 1:2 * p + 2], (rows, LANES))
        parts.append(jnp.where(low, left, right))
    return jnp.concatenate(parts, axis=1)


def lane_shift(v, first):
    return pltpu.roll(v, lax.rem(LANES - first, LANES), 1)


def project_kernel(x_hbm, w_hbm, an_hbm, db_hbm,
                   u_ref, loc_ref, hin_ref, bc_hbm, gl_hbm, qt_hbm, dec_hbm,
                   x_ref, wring, wdt_ref, an_ref, db_ref, bc_ref, gl_ref, qt_ref, dec_ref, isem, wsem, osem,
                   bt_ref, seg_dec, xw_ref, wst, uprev, drow, lsend, lall, s_own, rc, sx, rx, sy, ry, rf,
                   lsem, lrem, csem, crem, xsem, xrem, ysem, yrem, fsem, frem):
    step = pl.program_id(0)
    me = lax.axis_index("sp")
    tokens = x_ref.shape[0]
    segs = tokens // SEG
    tiles = s_own.shape[0]
    heads_at = 2 * tiles * TILE
    depth = x_ref.shape[1] // CHUNKS
    slots = wring.shape[0]
    small_loads = [
        pltpu.make_async_copy(db_hbm, db_ref, isem.at[0]),
        pltpu.make_async_copy(an_hbm, an_ref, isem.at[1]),
    ]

    def chunk_loads(q):
        part = slice(q * depth, (q + 1) * depth)
        return (pltpu.make_async_copy(x_hbm.at[:, part], x_ref.at[:, part], isem.at[2 + 2 * q]),
                pltpu.make_async_copy(w_hbm.at[part, heads_at:], wdt_ref.at[part, :], isem.at[3 + 2 * q]))

    def w_copy(at_step):
        slot = lax.rem(at_step, slots)
        first = pl.multiple_of(lax.rem(at_step + tiles, 2 * tiles) * TILE, TILE)
        return pltpu.make_async_copy(w_hbm.at[:, pl.ds(first, TILE)], wring.at[slot], wsem.at[slot])

    stores = [
        pltpu.make_async_copy(bc_ref, bc_hbm, osem.at[0]),
        pltpu.make_async_copy(gl_ref, gl_hbm, osem.at[1]),
        pltpu.make_async_copy(qt_ref, qt_hbm, osem.at[2]),
        pltpu.make_async_copy(dec_ref, dec_hbm, osem.at[3]),
    ]
    core = lax.rem(me, 2)
    xpos = lax.rem(me // 2, 2)
    ypos = me // 4
    peer_core = me + 1 - 2 * core
    peer_x = me + 2 - 4 * xpos
    peer_y = me + 4 - 8 * ypos
    barrier = pltpu.get_barrier_semaphore()

    def other(k):
        return lax.rem(me + k, 8)

    def log_copy(k):
        return pltpu.make_async_remote_copy(
            src_ref=lsend, dst_ref=lall.at[me], send_sem=lsem.at[k - 1], recv_sem=lrem.at[me],
            device_id={"sp": other(k)}, device_id_type=MESH)

    def remote(src, dst, send, recv, target):
        return pltpu.make_async_remote_copy(
            src_ref=src, dst_ref=dst, send_sem=send, recv_sem=recv,
            device_id={"sp": target}, device_id_type=MESH)

    def core_copy(c):
        return remote(s_own.at[c, 1 - core], rc.at[c], csem.at[c], crem.at[c], peer_core)

    def x_copy(c):
        return remote(sx.at[c], rx.at[c], xsem.at[c], xrem.at[c], peer_x)

    def y_copy(c):
        return remote(sy.at[c], ry.at[c], ysem.at[c], yrem.at[c], peer_y)

    def final_copy(c):
        return remote(sy.at[c], rf.at[c], fsem.at[c], frem.at[c], peer_core)

    def at_lag(lag):
        return jnp.logical_and(step >= lag, step < tiles + lag)

    def weigh(tile):
        weights = lane_shift(wst[...], tile * TILE_HEADS)
        for c in range(segs):
            rows = slice(c * SEG, (c + 1) * SEG)
            spread_rows = spread(weights[rows], TILE_HEADS // 2)
            xw_ref[rows, :] = (uprev[rows, :].astype(F32) * spread_rows).astype(BF16)

    def states(tile):
        dec = spread(lane_shift(seg_dec[...], tile * TILE_HEADS), TILE_HEADS // 2)
        state = dot32(bt_ref[:SEG, :], xw_ref[:SEG, :])
        for c in range(1, segs):
            rows = slice(c * SEG, (c + 1) * SEG)
            loc_ref[(c - 1) * STATE:c * STATE, :] = state
            state = dec[c:c + 1] * state + dot32(bt_ref[rows, :], xw_ref[rows, :])
        s_own[tile, 0] = state[:, :HALF]
        s_own[tile, 1] = state[:, HALF:]

    def project(keep):
        u = dot32(x_ref[...], wring[lax.rem(step, slots)]).astype(BF16)
        u_ref[...] = u
        if keep:
            uprev[...] = u

    @pl.when(step == 0)
    def _():
        for k in range(1, 8):
            pl.semaphore_signal(barrier, inc=1, device_id={"sp": other(k)}, device_id_type=MESH)
        for q in range(CHUNKS):
            for load in chunk_loads(q):
                load.start()
        for load in small_loads:
            load.start()
        for k in range(slots):
            w_copy(k).start()
        for load in small_loads:
            load.wait()
        last_columns = None
        for q in range(CHUNKS):
            for load in chunk_loads(q):
                load.wait()
            part = slice(q * depth, (q + 1) * depth)
            term = dot32(x_ref[:, part], wdt_ref[part, :])
            last_columns = term if last_columns is None else last_columns + term
        last_columns = last_columns.astype(BF16)
        bc = last_columns[:, :2 * STATE]
        bc_ref[...] = bc
        raw = last_columns[:, 2 * STATE:].astype(F32) + db_ref[...]
        dt = jnp.maximum(raw, 0.0) + jnp.log1p(jnp.exp(-jnp.abs(raw)))
        logs = dt * an_ref[...]
        tri = (lax.broadcasted_iota(jnp.int32, (SEG, SEG), 0)
               >= lax.broadcasted_iota(jnp.int32, (SEG, SEG), 1)).astype(F32)
        total = jnp.zeros((1, LANES), F32)
        row = lax.broadcasted_iota(jnp.int32, (8, LANES), 0)
        dec = jnp.zeros((8, LANES), F32)
        before = jnp.zeros((8, LANES), F32)
        for c in range(segs):
            rows = slice(c * SEG, (c + 1) * SEG)
            cum = jnp.dot(tri, logs[rows], precision=lax.Precision.HIGHEST, preferred_element_type=F32)
            last = cum[SEG - 1:SEG]
            wst[rows, :] = jnp.exp(last - cum) * dt[rows]
            gl_ref[rows, :] = cum * LOG2E
            qt_ref[rows, :] = jnp.transpose(cum * LOG2E - jnp.log2(dt[rows]))
            bt_ref[rows, :] = jnp.transpose(bc[rows, :STATE].astype(F32)).astype(BF16)
            dec = jnp.where(row == c, jnp.exp(last), dec)
            before = jnp.where(row == c, jnp.exp(total), before)
            total = total + last
        seg_dec[...] = dec
        dec_ref[...] = before
        lsend[...] = jnp.broadcast_to(total, (8, LANES))

    def s_of(mine, c):
        return jnp.where(mine, s_own[c, core], rc[c])

    @pl.when(step == 2)
    def _():
        pl.semaphore_wait(barrier, 7)
        for store in stores:
            store.start()
        for k in range(1, 8):
            log_copy(k).start()
        lall[me] = lsend[...]

    @pl.when(at_lag(3))
    def _():
        core_copy(step - 3).start()

    @pl.when(step == 4)
    def _():
        for k in range(1, 8):
            log_copy(k).wait_send()
            source = other(k)
            pltpu.make_async_remote_copy(
                src_ref=lsend, dst_ref=lall.at[source], send_sem=lsem.at[k - 1], recv_sem=lrem.at[source],
                device_id={"sp": source}, device_id_type=MESH).wait_recv()
        chip = ypos * 4
        row = lax.broadcasted_iota(jnp.int32, (8, LANES), 0)
        logs = jnp.where(row == 0, lall[me - core + 1], 0.0)
        logs = jnp.where(row == 1, lall[chip + 2] + lall[chip + 3], logs)
        logs = jnp.where(jnp.logical_and(row == 2, xpos == 1), lall[chip] + lall[chip + 1], logs)
        logs = jnp.where(row == 3, lall[me - core], logs)
        decays = jnp.exp(logs)
        for c in range(tiles):
            drow[c] = spread(lane_shift(decays, c * TILE_HEADS + core * (TILE_HEADS // 2)), 2)

    @pl.when(at_lag(4))
    def _():
        c = step - 4
        core_copy(c).wait()
        sx[c] = drow[c, 0:1] * s_of(core == 0, c) + s_of(core == 1, c)

    @pl.when(at_lag(5))
    def _():
        x_copy(step - 5).start()

    @pl.when(at_lag(LAG_X))
    def _():
        c = step - LAG_X
        x_copy(c).wait()
        mine, got = sx[c], rx[c]
        early = jnp.where(xpos == 0, mine, got)
        late = jnp.where(xpos == 0, got, mine)
        sy[c] = drow[c, 1:2] * early + late

    @pl.when(at_lag(LAG_X + 1))
    def _():
        y_copy(step - LAG_X - 1).start()

    @pl.when(at_lag(LAG_Y))
    def _():
        c = step - LAG_Y
        y_copy(c).wait()
        before = jnp.where(xpos == 1, rx[c], 0.0) + jnp.where(ypos == 1, drow[c, 2:3] * ry[c], 0.0)
        after = drow[c, 3:4] * before + s_of(core == 0, c)
        sx[c] = jnp.where(core == 0, before, after)
        sy[c] = jnp.where(core == 0, after, before)

    @pl.when(at_lag(LAG_Y + 1))
    def _():
        final_copy(step - LAG_Y - 1).start()

    @pl.when(at_lag(LAG_Y + 2))
    def _():
        c = step - LAG_Y - 2
        final_copy(c).wait()
        mine, got = sx[c], rf[c]
        hin_ref[:, :HALF] = jnp.where(core == 0, mine, got)
        hin_ref[:, HALF:] = jnp.where(core == 0, got, mine)

    with_state = jnp.logical_and(step >= 1, step <= tiles + 1)

    @pl.when(with_state)
    def _():
        w_copy(step).wait()
        states(jnp.maximum(step - 2, 0))
        weigh(step - 1)
        project(True)

    @pl.when(step == 0)
    def _():
        w_copy(step).wait()
        project(True)

    @pl.when(step > tiles + 1)
    def _():
        w_copy(step).wait()
        project(False)

    @pl.when(step + slots < 2 * tiles)
    def _():
        w_copy(step + slots).start()

    @pl.when(step == 2 * tiles - 1)
    def _():
        for store in stores:
            store.wait()


def mix_kernel(z_ref, xs_ref, loc_ref, h_ref, bc_ref, gl_ref, qt_ref, dec_ref, ds_ref, w_hbm, x_hbm,
               out_hbm, acc, gated_a, gated_b, scores, wbuf, out_ref, w_sem, x_sem, o_sem):
    step = pl.program_id(0)
    steps = pl.num_programs(0)
    tokens, d_model = acc.shape
    segs = tokens // SEG
    slots = wbuf.shape[0]
    groups = w_hbm.shape[0] // TILE
    x_copy = pltpu.make_async_copy(x_hbm, out_ref, x_sem)

    def w_copy(group):
        slot = lax.rem(group, slots)
        first = pl.multiple_of(group * TILE, TILE)
        return pltpu.make_async_copy(w_hbm.at[pl.ds(first, TILE), :], wbuf.at[slot], w_sem.at[slot])

    def w_next(group):
        @pl.when(group + slots < groups)
        def _():
            w_copy(group + slots).start()

    def dot_slice(k, source, group):
        cols = slice(k * TILE, (k + 1) * TILE)
        acc[:, cols] += dot32(source[...], wbuf[lax.rem(group, slots), :, cols])

    def group_outputs(half, target, big):
        base = half * TILE
        first = (2 * step + half) * TILE_HEADS
        gl = lane_shift(gl_ref[...], first)
        dec = spread(lane_shift(dec_ref[...], first), TILE_HEADS // 2)
        skip = spread(lane_shift(jnp.broadcast_to(ds_ref[...], (8, LANES)), first), TILE_HEADS // 2)[:1]
        causal = (lax.broadcasted_iota(jnp.int32, (SEG, SEG), 0)
                  >= lax.broadcasted_iota(jnp.int32, (SEG, SEG), 1))
        low = lax.broadcasted_iota(jnp.int32, (SEG, LANES), 1) < HEAD_DIM
        zero = jnp.zeros((SEG, LANES), BF16)
        pending = None
        unit = 0
        for c in range(segs):
            rows = slice(c * SEG, (c + 1) * SEG)
            state = h_ref[:, base:base + TILE]
            if c > 0:
                state = dec[c:c + 1] * state + loc_ref[(c - 1) * STATE:c * STATE, base:base + TILE]
            y_state = dot32(bc_ref[rows, STATE:], state.astype(BF16))
            q_rows = qt_ref[pl.ds(pl.multiple_of(c * SEG + first, TILE_HEADS), TILE_HEADS), :]
            for p in range(TILE_HEADS // 2):
                cols = slice(base + p * LANES, base + (p + 1) * LANES)
                sc = scores[rows, :]
                col_a = jnp.broadcast_to(gl[rows, 2 * p:2 * p + 1], (SEG, LANES))
                col_b = jnp.broadcast_to(gl[rows, 2 * p + 1:2 * p + 2], (SEG, LANES))
                g_a = jnp.where(causal, sc * jnp.exp2(col_a - q_rows[2 * p:2 * p + 1]), 0.0).astype(BF16)
                g_b = jnp.where(causal, sc * jnp.exp2(col_b - q_rows[2 * p + 1:2 * p + 2]), 0.0).astype(BF16)
                xp = xs_ref[rows, cols]
                rhs = jnp.concatenate([jnp.where(low, xp, zero), jnp.where(low, zero, xp)], axis=0)
                if unit % 2 == 0 and big is not None:
                    dot_slice(unit // 2, *big)
                y = dot32(jnp.concatenate([g_a, g_b], axis=1), rhs)
                if pending is not None:
                    pending()

                def pending(y=y, rows=rows, cols=cols, p=p, y_state=y_state, col_a=col_a, col_b=col_b):
                    here = slice(p * LANES, (p + 1) * LANES)
                    total = y + y_state[:, here] * jnp.exp2(jnp.where(low, col_a, col_b))
                    total = total + skip[:, here] * xs_ref[rows, cols].astype(F32)
                    z = z_ref[rows, cols].astype(F32)
                    target[rows, here] = (total * (z / (1.0 + jnp.exp(-z)))).astype(BF16)
                unit += 1
        pending()

    @pl.when(step == 0)
    def _():
        for group in range(slots):
            w_copy(group).start()
        x_copy.start()
        acc[...] = jnp.zeros_like(acc)
        for c in range(segs):
            rows = slice(c * SEG, (c + 1) * SEG)
            scores[rows, :] = lax.dot_general(bc_ref[rows, STATE:], bc_ref[rows, :STATE],
                                              (((1,), (1,)), ((), ())), preferred_element_type=F32)
        group_outputs(0, gated_a, None)

    @pl.when(jnp.logical_and(step > 0, step < steps - 1))
    def _():
        w_copy(2 * step - 1).wait()
        group_outputs(0, gated_a, (gated_b, 2 * step - 1))
        w_next(2 * step - 1)

    @pl.when(step < steps - 1)
    def _():
        w_copy(2 * step).wait()
        group_outputs(1, gated_b, (gated_a, 2 * step))
        w_next(2 * step)

    @pl.when(step == steps - 1)
    def _():
        x_copy.wait()
        w_copy(groups - 1).wait()
        copies = []
        for k in range(d_model // (2 * TILE)):
            cols = slice(2 * k * TILE, 2 * (k + 1) * TILE)
            total = acc[:, cols] + dot32(gated_b[...], wbuf[(groups - 1) % slots, :, cols])
            out_ref[:, cols] = (out_ref[:, cols].astype(F32) + total).astype(BF16)
            copies.append(pltpu.make_async_copy(out_ref.at[:, cols], out_hbm.at[:, cols], o_sem.at[k]))
            copies[-1].start()
        for copy in copies:
            copy.wait()


def solution(mesh):
    row_spec = P(("dp", "sp"), None)

    def local_mixer(x_loc, w_in, a_neg, dt_bias, d_skip, w_out):
        tokens, d_model = x_loc.shape
        inner = w_out.shape[0]
        heads = a_neg.shape[0]
        tiles = inner // TILE
        segs = tokens // SEG
        assert mesh.shape["sp"] == 8 and heads == LANES and inner == heads * HEAD_DIM
        assert tiles >= LAG_Y + 2
        def fixed(shape):
            return pl.BlockSpec(shape, lambda i: (0,) * len(shape), pipeline_mode=pl.Buffered(1))

        half = (tiles, STATE, HALF)
        sems = pltpu.SemaphoreType.DMA((tiles,))
        any_space = pl.BlockSpec(memory_space=pl.ANY)
        u, loc, h_in, bc, gl, qt, dec = pl.pallas_call(
            project_kernel,
            grid=(2 * tiles,),
            out_shape=[
                jax.ShapeDtypeStruct((tokens, 2 * inner), BF16),
                jax.ShapeDtypeStruct(((segs - 1) * STATE, inner), F32),
                jax.ShapeDtypeStruct((STATE, inner), F32),
                jax.ShapeDtypeStruct((tokens, 2 * STATE), BF16),
                jax.ShapeDtypeStruct((tokens, heads), F32),
                jax.ShapeDtypeStruct((segs * heads, SEG), F32),
                jax.ShapeDtypeStruct((8, heads), F32),
            ],
            in_specs=[
                any_space, any_space, any_space, any_space,
            ],
            out_specs=[
                pl.BlockSpec((tokens, TILE), lambda i: (0, lax.rem(i + tiles, 2 * tiles))),
                pl.BlockSpec(((segs - 1) * STATE, TILE), lambda i: (0, jnp.clip(i - 2, 0, tiles - 1))),
                pl.BlockSpec((STATE, TILE), lambda i: (0, jnp.maximum(i - (LAG_Y + 2), 0))),
                any_space, any_space, any_space, any_space,
            ],
            scratch_shapes=[
                pltpu.VMEM((tokens, d_model), BF16),
                pltpu.VMEM((3, d_model, TILE), BF16),
                pltpu.VMEM((d_model, 2 * STATE + heads), BF16),
                pltpu.VMEM((1, heads), F32), pltpu.VMEM((1, heads), F32),
                pltpu.VMEM((tokens, 2 * STATE), BF16),
                pltpu.VMEM((tokens, heads), F32),
                pltpu.VMEM((segs * heads, SEG), F32),
                pltpu.VMEM((8, heads), F32),
                pltpu.SemaphoreType.DMA((2 + 2 * CHUNKS,)), pltpu.SemaphoreType.DMA((3,)), pltpu.SemaphoreType.DMA((4,)),
                pltpu.VMEM((segs * STATE, SEG), BF16),
                pltpu.VMEM((8, heads), F32),
                pltpu.VMEM((tokens, TILE), BF16),
                pltpu.VMEM((tokens, heads), F32),
                pltpu.VMEM((tokens, TILE), BF16),
                pltpu.VMEM((tiles, 8, HALF), F32),
                pltpu.VMEM((8, heads), F32),
                pltpu.VMEM((8, 8, heads), F32),
                pltpu.VMEM((tiles, 2, STATE, HALF), F32),
                pltpu.VMEM(half, F32), pltpu.VMEM(half, F32), pltpu.VMEM(half, F32),
                pltpu.VMEM(half, F32), pltpu.VMEM(half, F32), pltpu.VMEM(half, F32),
                pltpu.SemaphoreType.DMA((7,)), pltpu.SemaphoreType.DMA((8,)),
                sems, sems, sems, sems, sems, sems, sems, sems,
            ],
            compiler_params=pltpu.CompilerParams(
                dimension_semantics=("arbitrary",), collective_id=0, has_side_effects=True,
                vmem_limit_bytes=60 * 1024 * 1024),
            cost_estimate=pl.CostEstimate(flops=2 * tokens * d_model * w_in.shape[1],
                                          bytes_accessed=2 * w_in.size, transcendentals=0),
            name="project",
        )(x_loc, w_in, a_neg.reshape(1, heads), dt_bias.reshape(1, heads))

        last = tiles // 2 - 1
        return pl.pallas_call(
            mix_kernel,
            grid=(tiles // 2 + 1,),
            out_shape=jax.ShapeDtypeStruct((tokens, d_model), BF16),
            in_specs=[
                pl.BlockSpec((tokens, 2 * TILE), lambda i: (0, jnp.minimum(i, last))),
                pl.BlockSpec((tokens, 2 * TILE), lambda i: (0, jnp.minimum(i, last) + tiles // 2)),
                pl.BlockSpec(((segs - 1) * STATE, 2 * TILE), lambda i: (0, jnp.minimum(i, last))),
                pl.BlockSpec((STATE, 2 * TILE), lambda i: (0, jnp.minimum(i, last))),
                fixed((tokens, 2 * STATE)), fixed((tokens, heads)),
                fixed((segs * heads, SEG)), fixed((8, heads)), fixed((1, heads)),
                any_space, any_space,
            ],
            out_specs=any_space,
            scratch_shapes=[
                pltpu.VMEM((tokens, d_model), F32),
                pltpu.VMEM((tokens, TILE), BF16),
                pltpu.VMEM((tokens, TILE), BF16),
                pltpu.VMEM((tokens, SEG), F32),
                pltpu.VMEM((4, TILE, d_model), BF16),
                pltpu.VMEM((tokens, d_model), BF16),
                pltpu.SemaphoreType.DMA((4,)),
                pltpu.SemaphoreType.DMA(()),
                pltpu.SemaphoreType.DMA((d_model // (2 * TILE),)),
            ],
            compiler_params=pltpu.CompilerParams(
                dimension_semantics=("arbitrary",), vmem_limit_bytes=62 * 1024 * 1024),
            cost_estimate=pl.CostEstimate(flops=2 * tokens * d_model * inner,
                                          bytes_accessed=2 * w_out.size, transcendentals=0),
            name="mix",
        )(u, u, loc, h_in, bc, gl, qt, dec, d_skip.reshape(1, heads), w_out, x_loc)

    return jax.shard_map(local_mixer, mesh=mesh, in_specs=(row_spec, P(), P(), P(), P(), P()),
                         out_specs=row_spec, check_vma=False)
```

```python
import jax
import jax.numpy as jnp
from jax import lax
from jax.experimental import pallas as pl
from jax.experimental.pallas import tpu as pltpu
from jax.sharding import PartitionSpec as P

SEG = 128
HEAD_DIM = 64
STATE = 128
TILE = 512
HALF = TILE // 2
TILE_HEADS = TILE // HEAD_DIM
LANES = 128
CHUNKS = 4
LAG_X = 9
LAG_Y = 14
LOG2E = 1.4426950408889634
MESH = pl.DeviceIdType.MESH
BF16 = jnp.bfloat16
F32 = jnp.float32


def dot32(a, b):
    return jnp.dot(a, b, preferred_element_type=F32)


def spread(v, pairs):
    rows = v.shape[0]
    low = lax.broadcasted_iota(jnp.int32, (rows, LANES), 1) < HEAD_DIM
    parts = []
    for p in range(pairs):
        left = jnp.broadcast_to(v[:, 2 * p:2 * p + 1], (rows, LANES))
        right = jnp.broadcast_to(v[:, 2 * p + 1:2 * p + 2], (rows, LANES))
        parts.append(jnp.where(low, left, right))
    return jnp.concatenate(parts, axis=1)


def lane_shift(v, first):
    return pltpu.roll(v, lax.rem(LANES - first, LANES), 1)


def project_kernel(x_hbm, w_hbm, an_hbm, db_hbm,
                   u_ref, loc_ref, hin_ref, bc_hbm, gl_hbm, qt_hbm, dec_hbm,
                   x_ref, wring, wdt_ref, an_ref, db_ref, bc_ref, gl_ref, qt_ref, dec_ref, isem, wsem, osem,
                   bt_ref, seg_dec, xw_ref, wst, uprev, drow, lsend, lall, s_own, rc, sx, rx, sy, ry, rf,
                   lsem, lrem, csem, crem, xsem, xrem, ysem, yrem, fsem, frem):
    step = pl.program_id(0)
    me = lax.axis_index("sp")
    tokens = x_ref.shape[0]
    segs = tokens // SEG
    tiles = s_own.shape[0]
    heads_at = 2 * tiles * TILE
    depth = x_ref.shape[1] // CHUNKS
    slots = wring.shape[0]
    small_loads = [
        pltpu.make_async_copy(db_hbm, db_ref, isem.at[0]),
        pltpu.make_async_copy(an_hbm, an_ref, isem.at[1]),
    ]

    def chunk_loads(q):
        part = slice(q * depth, (q + 1) * depth)
        return (pltpu.make_async_copy(x_hbm.at[:, part], x_ref.at[:, part], isem.at[2 + 2 * q]),
                pltpu.make_async_copy(w_hbm.at[part, heads_at:], wdt_ref.at[part, :], isem.at[3 + 2 * q]))

    def w_copy(at_step):
        slot = lax.rem(at_step, slots)
        first = pl.multiple_of(lax.rem(at_step + tiles, 2 * tiles) * TILE, TILE)
        return pltpu.make_async_copy(w_hbm.at[:, pl.ds(first, TILE)], wring.at[slot], wsem.at[slot])

    stores = [
        pltpu.make_async_copy(bc_ref, bc_hbm, osem.at[0]),
        pltpu.make_async_copy(gl_ref, gl_hbm, osem.at[1]),
        pltpu.make_async_copy(qt_ref, qt_hbm, osem.at[2]),
        pltpu.make_async_copy(dec_ref, dec_hbm, osem.at[3]),
    ]
    core = lax.rem(me, 2)
    xpos = lax.rem(me // 2, 2)
    ypos = me // 4
    peer_core = me + 1 - 2 * core
    peer_x = me + 2 - 4 * xpos
    peer_y = me + 4 - 8 * ypos
    barrier = pltpu.get_barrier_semaphore()

    def other(k):
        return lax.rem(me + k, 8)

    def log_copy(k):
        return pltpu.make_async_remote_copy(
            src_ref=lsend, dst_ref=lall.at[me], send_sem=lsem.at[k - 1], recv_sem=lrem.at[me],
            device_id={"sp": other(k)}, device_id_type=MESH)

    def remote(src, dst, send, recv, target):
        return pltpu.make_async_remote_copy(
            src_ref=src, dst_ref=dst, send_sem=send, recv_sem=recv,
            device_id={"sp": target}, device_id_type=MESH)

    def core_copy(c):
        return remote(s_own.at[c, 1 - core], rc.at[c], csem.at[c], crem.at[c], peer_core)

    def x_copy(c):
        return remote(sx.at[c], rx.at[c], xsem.at[c], xrem.at[c], peer_x)

    def y_copy(c):
        return remote(sy.at[c], ry.at[c], ysem.at[c], yrem.at[c], peer_y)

    def final_copy(c):
        return remote(sy.at[c], rf.at[c], fsem.at[c], frem.at[c], peer_core)

    def at_lag(lag):
        return jnp.logical_and(step >= lag, step < tiles + lag)

    def weigh(tile):
        weights = lane_shift(wst[...], tile * TILE_HEADS)
        for c in range(segs):
            rows = slice(c * SEG, (c + 1) * SEG)
            spread_rows = spread(weights[rows], TILE_HEADS // 2)
            xw_ref[rows, :] = (uprev[rows, :].astype(F32) * spread_rows).astype(BF16)

    def states(tile):
        dec = spread(lane_shift(seg_dec[...], tile * TILE_HEADS), TILE_HEADS // 2)
        state = dot32(bt_ref[:SEG, :], xw_ref[:SEG, :])
        for c in range(1, segs):
            rows = slice(c * SEG, (c + 1) * SEG)
            loc_ref[(c - 1) * STATE:c * STATE, :] = state
            state = dec[c:c + 1] * state + dot32(bt_ref[rows, :], xw_ref[rows, :])
        s_own[tile, 0] = state[:, :HALF]
        s_own[tile, 1] = state[:, HALF:]

    def project(keep):
        u = dot32(x_ref[...], wring[lax.rem(step, slots)]).astype(BF16)
        u_ref[...] = u
        if keep:
            uprev[...] = u

    @pl.when(step == 0)
    def _():
        for k in range(1, 8):
            pl.semaphore_signal(barrier, inc=1, device_id={"sp": other(k)}, device_id_type=MESH)
        for q in range(CHUNKS):
            for load in chunk_loads(q):
                load.start()
        for load in small_loads:
            load.start()
        for k in range(slots):
            w_copy(k).start()
        for load in small_loads:
            load.wait()
        last_columns = None
        for q in range(CHUNKS):
            for load in chunk_loads(q):
                load.wait()
            part = slice(q * depth, (q + 1) * depth)
            term = dot32(x_ref[:, part], wdt_ref[part, :])
            last_columns = term if last_columns is None else last_columns + term
        last_columns = last_columns.astype(BF16)
        bc = last_columns[:, :2 * STATE]
        bc_ref[...] = bc
        raw = last_columns[:, 2 * STATE:].astype(F32) + db_ref[...]
        dt = jnp.maximum(raw, 0.0) + jnp.log1p(jnp.exp(-jnp.abs(raw)))
        logs = dt * an_ref[...]
        tri = (lax.broadcasted_iota(jnp.int32, (SEG, SEG), 0)
               >= lax.broadcasted_iota(jnp.int32, (SEG, SEG), 1)).astype(F32)
        total = jnp.zeros((1, LANES), F32)
        row = lax.broadcasted_iota(jnp.int32, (8, LANES), 0)
        dec = jnp.zeros((8, LANES), F32)
        before = jnp.zeros((8, LANES), F32)
        for c in range(segs):
            rows = slice(c * SEG, (c + 1) * SEG)
            cum = jnp.dot(tri, logs[rows], precision=lax.Precision.HIGHEST, preferred_element_type=F32)
            last = cum[SEG - 1:SEG]
            wst[rows, :] = jnp.exp(last - cum) * dt[rows]
            gl_ref[rows, :] = cum * LOG2E
            qt_ref[rows, :] = jnp.transpose(cum * LOG2E - jnp.log2(dt[rows]))
            bt_ref[rows, :] = jnp.transpose(bc[rows, :STATE].astype(F32)).astype(BF16)
            dec = jnp.where(row == c, jnp.exp(last), dec)
            before = jnp.where(row == c, jnp.exp(total), before)
            total = total + last
        seg_dec[...] = dec
        dec_ref[...] = before
        lsend[...] = jnp.broadcast_to(total, (8, LANES))

    def s_of(mine, c):
        return jnp.where(mine, s_own[c, core], rc[c])

    @pl.when(step == 2)
    def _():
        pl.semaphore_wait(barrier, 7)
        for store in stores:
            store.start()
        for k in range(1, 8):
            log_copy(k).start()
        lall[me] = lsend[...]

    @pl.when(at_lag(3))
    def _():
        core_copy(step - 3).start()

    @pl.when(step == 4)
    def _():
        for k in range(1, 8):
            log_copy(k).wait_send()
            source = other(k)
            pltpu.make_async_remote_copy(
                src_ref=lsend, dst_ref=lall.at[source], send_sem=lsem.at[k - 1], recv_sem=lrem.at[source],
                device_id={"sp": source}, device_id_type=MESH).wait_recv()
        chip = ypos * 4
        row = lax.broadcasted_iota(jnp.int32, (8, LANES), 0)
        logs = jnp.where(row == 0, lall[me - core + 1], 0.0)
        logs = jnp.where(row == 1, lall[chip + 2] + lall[chip + 3], logs)
        logs = jnp.where(jnp.logical_and(row == 2, xpos == 1), lall[chip] + lall[chip + 1], logs)
        logs = jnp.where(row == 3, lall[me - core], logs)
        decays = jnp.exp(logs)
        for c in range(tiles):
            drow[c] = spread(lane_shift(decays, c * TILE_HEADS + core * (TILE_HEADS // 2)), 2)

    @pl.when(at_lag(4))
    def _():
        c = step - 4
        core_copy(c).wait()
        sx[c] = drow[c, 0:1] * s_of(core == 0, c) + s_of(core == 1, c)

    @pl.when(at_lag(5))
    def _():
        x_copy(step - 5).start()

    @pl.when(at_lag(LAG_X))
    def _():
        c = step - LAG_X
        x_copy(c).wait()
        mine, got = sx[c], rx[c]
        early = jnp.where(xpos == 0, mine, got)
        late = jnp.where(xpos == 0, got, mine)
        sy[c] = drow[c, 1:2] * early + late

    @pl.when(at_lag(LAG_X + 1))
    def _():
        y_copy(step - LAG_X - 1).start()

    @pl.when(at_lag(LAG_Y))
    def _():
        c = step - LAG_Y
        y_copy(c).wait()
        before = jnp.where(xpos == 1, rx[c], 0.0) + jnp.where(ypos == 1, drow[c, 2:3] * ry[c], 0.0)
        after = drow[c, 3:4] * before + s_of(core == 0, c)
        sx[c] = jnp.where(core == 0, before, after)
        sy[c] = jnp.where(core == 0, after, before)

    @pl.when(at_lag(LAG_Y + 1))
    def _():
        final_copy(step - LAG_Y - 1).start()

    @pl.when(at_lag(LAG_Y + 2))
    def _():
        c = step - LAG_Y - 2
        final_copy(c).wait()
        mine, got = sx[c], rf[c]
        hin_ref[:, :HALF] = jnp.where(core == 0, mine, got)
        hin_ref[:, HALF:] = jnp.where(core == 0, got, mine)

    with_state = jnp.logical_and(step >= 1, step <= tiles + 1)

    @pl.when(with_state)
    def _():
        w_copy(step).wait()
        states(jnp.maximum(step - 2, 0))
        weigh(step - 1)
        project(True)

    @pl.when(step == 0)
    def _():
        w_copy(step).wait()
        project(True)

    @pl.when(step > tiles + 1)
    def _():
        w_copy(step).wait()
        project(False)

    @pl.when(step + slots < 2 * tiles)
    def _():
        w_copy(step + slots).start()

    @pl.when(step == 2 * tiles - 1)
    def _():
        for store in stores:
            store.wait()


def mix_kernel(z_ref, xs_ref, loc_ref, h_ref, bc_ref, gl_ref, qt_ref, dec_ref, ds_ref, w_hbm, x_hbm,
               out_hbm, acc, gated_a, gated_b, scores, wbuf, out_ref, w_sem, x_sem, o_sem):
    step = pl.program_id(0)
    steps = pl.num_programs(0)
    tokens, d_model = acc.shape
    segs = tokens // SEG
    slots = wbuf.shape[0]
    groups = w_hbm.shape[0] // TILE
    x_copy = pltpu.make_async_copy(x_hbm, out_ref, x_sem)

    def w_copy(group):
        slot = lax.rem(group, slots)
        first = pl.multiple_of(group * TILE, TILE)
        return pltpu.make_async_copy(w_hbm.at[pl.ds(first, TILE), :], wbuf.at[slot], w_sem.at[slot])

    def w_next(group):
        @pl.when(group + slots < groups)
        def _():
            w_copy(group + slots).start()

    def dot_slice(k, source, group):
        cols = slice(k * HALF, (k + 1) * HALF)
        acc[:, cols] += dot32(source[...], wbuf[lax.rem(group, slots), :, cols])

    def group_outputs(half, target, big):
        base = half * TILE
        first = (2 * step + half) * TILE_HEADS
        gl = lane_shift(gl_ref[...], first)
        dec = spread(lane_shift(dec_ref[...], first), TILE_HEADS // 2)
        skip = spread(lane_shift(jnp.broadcast_to(ds_ref[...], (8, LANES)), first), TILE_HEADS // 2)[:1]
        causal = (lax.broadcasted_iota(jnp.int32, (SEG, SEG), 0)
                  >= lax.broadcasted_iota(jnp.int32, (SEG, SEG), 1))
        low = lax.broadcasted_iota(jnp.int32, (SEG, LANES), 1) < HEAD_DIM
        zero = jnp.zeros((SEG, LANES), BF16)
        pending = None
        unit = 0
        for c in range(segs):
            rows = slice(c * SEG, (c + 1) * SEG)
            state = h_ref[:, base:base + TILE]
            if c > 0:
                state = dec[c:c + 1] * state + loc_ref[(c - 1) * STATE:c * STATE, base:base + TILE]
            y_state = dot32(bc_ref[rows, STATE:], state.astype(BF16))
            q_rows = qt_ref[pl.ds(pl.multiple_of(c * SEG + first, TILE_HEADS), TILE_HEADS), :]
            for p in range(TILE_HEADS // 2):
                cols = slice(base + p * LANES, base + (p + 1) * LANES)
                sc = scores[rows, :]
                col_a = jnp.broadcast_to(gl[rows, 2 * p:2 * p + 1], (SEG, LANES))
                col_b = jnp.broadcast_to(gl[rows, 2 * p + 1:2 * p + 2], (SEG, LANES))
                g_a = jnp.where(causal, sc * jnp.exp2(col_a - q_rows[2 * p:2 * p + 1]), 0.0).astype(BF16)
                g_b = jnp.where(causal, sc * jnp.exp2(col_b - q_rows[2 * p + 1:2 * p + 2]), 0.0).astype(BF16)
                xp = xs_ref[rows, cols]
                rhs = jnp.concatenate([jnp.where(low, xp, zero), jnp.where(low, zero, xp)], axis=0)
                if big is not None:
                    dot_slice(unit, *big)
                y = dot32(jnp.concatenate([g_a, g_b], axis=1), rhs)
                if pending is not None:
                    pending()

                def pending(y=y, rows=rows, cols=cols, p=p, y_state=y_state, col_a=col_a, col_b=col_b):
                    here = slice(p * LANES, (p + 1) * LANES)
                    total = y + y_state[:, here] * jnp.exp2(jnp.where(low, col_a, col_b))
                    total = total + skip[:, here] * xs_ref[rows, cols].astype(F32)
                    z = z_ref[rows, cols].astype(F32)
                    target[rows, here] = (total * (z / (1.0 + jnp.exp(-z)))).astype(BF16)
                unit += 1
        pending()

    @pl.when(step == 0)
    def _():
        for group in range(slots):
            w_copy(group).start()
        x_copy.start()
        acc[...] = jnp.zeros_like(acc)
        for c in range(segs):
            rows = slice(c * SEG, (c + 1) * SEG)
            scores[rows, :] = lax.dot_general(bc_ref[rows, STATE:], bc_ref[rows, :STATE],
                                              (((1,), (1,)), ((), ())), preferred_element_type=F32)
        group_outputs(0, gated_a, None)
        w_copy(0).wait()
        group_outputs(1, gated_b, (gated_a, 0))
        w_next(0)

    @pl.when(jnp.logical_and(step > 0, step < steps - 1))
    def _():
        w_copy(2 * step - 1).wait()
        w_copy(2 * step).wait()
        group_outputs(0, gated_a, (gated_b, 2 * step - 1))
        group_outputs(1, gated_b, (gated_a, 2 * step))
        w_next(2 * step - 1)
        w_next(2 * step)

    @pl.when(step == steps - 1)
    def _():
        x_copy.wait()
        w_copy(groups - 1).wait()
        copies = []
        for k in range(d_model // (2 * TILE)):
            cols = slice(2 * k * TILE, 2 * (k + 1) * TILE)
            total = acc[:, cols] + dot32(gated_b[...], wbuf[(groups - 1) % slots, :, cols])
            out_ref[:, cols] = (out_ref[:, cols].astype(F32) + total).astype(BF16)
            copies.append(pltpu.make_async_copy(out_ref.at[:, cols], out_hbm.at[:, cols], o_sem.at[k]))
            copies[-1].start()
        for copy in copies:
            copy.wait()


def solution(mesh):
    row_spec = P(("dp", "sp"), None)

    def local_mixer(x_loc, w_in, a_neg, dt_bias, d_skip, w_out):
        tokens, d_model = x_loc.shape
        inner = w_out.shape[0]
        heads = a_neg.shape[0]
        tiles = inner // TILE
        segs = tokens // SEG
        assert mesh.shape["sp"] == 8 and heads == LANES and inner == heads * HEAD_DIM
        assert tiles >= LAG_Y + 2
        def fixed(shape):
            return pl.BlockSpec(shape, lambda i: (0,) * len(shape), pipeline_mode=pl.Buffered(1))

        half = (tiles, STATE, HALF)
        sems = pltpu.SemaphoreType.DMA((tiles,))
        any_space = pl.BlockSpec(memory_space=pl.ANY)
        u, loc, h_in, bc, gl, qt, dec = pl.pallas_call(
            project_kernel,
            grid=(2 * tiles,),
            out_shape=[
                jax.ShapeDtypeStruct((tokens, 2 * inner), BF16),
                jax.ShapeDtypeStruct(((segs - 1) * STATE, inner), F32),
                jax.ShapeDtypeStruct((STATE, inner), F32),
                jax.ShapeDtypeStruct((tokens, 2 * STATE), BF16),
                jax.ShapeDtypeStruct((tokens, heads), F32),
                jax.ShapeDtypeStruct((segs * heads, SEG), F32),
                jax.ShapeDtypeStruct((8, heads), F32),
            ],
            in_specs=[
                any_space, any_space, any_space, any_space,
            ],
            out_specs=[
                pl.BlockSpec((tokens, TILE), lambda i: (0, lax.rem(i + tiles, 2 * tiles))),
                pl.BlockSpec(((segs - 1) * STATE, TILE), lambda i: (0, jnp.clip(i - 2, 0, tiles - 1))),
                pl.BlockSpec((STATE, TILE), lambda i: (0, jnp.maximum(i - (LAG_Y + 2), 0))),
                any_space, any_space, any_space, any_space,
            ],
            scratch_shapes=[
                pltpu.VMEM((tokens, d_model), BF16),
                pltpu.VMEM((3, d_model, TILE), BF16),
                pltpu.VMEM((d_model, 2 * STATE + heads), BF16),
                pltpu.VMEM((1, heads), F32), pltpu.VMEM((1, heads), F32),
                pltpu.VMEM((tokens, 2 * STATE), BF16),
                pltpu.VMEM((tokens, heads), F32),
                pltpu.VMEM((segs * heads, SEG), F32),
                pltpu.VMEM((8, heads), F32),
                pltpu.SemaphoreType.DMA((2 + 2 * CHUNKS,)), pltpu.SemaphoreType.DMA((3,)), pltpu.SemaphoreType.DMA((4,)),
                pltpu.VMEM((segs * STATE, SEG), BF16),
                pltpu.VMEM((8, heads), F32),
                pltpu.VMEM((tokens, TILE), BF16),
                pltpu.VMEM((tokens, heads), F32),
                pltpu.VMEM((tokens, TILE), BF16),
                pltpu.VMEM((tiles, 8, HALF), F32),
                pltpu.VMEM((8, heads), F32),
                pltpu.VMEM((8, 8, heads), F32),
                pltpu.VMEM((tiles, 2, STATE, HALF), F32),
                pltpu.VMEM(half, F32), pltpu.VMEM(half, F32), pltpu.VMEM(half, F32),
                pltpu.VMEM(half, F32), pltpu.VMEM(half, F32), pltpu.VMEM(half, F32),
                pltpu.SemaphoreType.DMA((7,)), pltpu.SemaphoreType.DMA((8,)),
                sems, sems, sems, sems, sems, sems, sems, sems,
            ],
            compiler_params=pltpu.CompilerParams(
                dimension_semantics=("arbitrary",), collective_id=0, has_side_effects=True,
                vmem_limit_bytes=60 * 1024 * 1024),
            cost_estimate=pl.CostEstimate(flops=2 * tokens * d_model * w_in.shape[1],
                                          bytes_accessed=2 * w_in.size, transcendentals=0),
            name="project",
        )(x_loc, w_in, a_neg.reshape(1, heads), dt_bias.reshape(1, heads))

        last = tiles // 2 - 1
        return pl.pallas_call(
            mix_kernel,
            grid=(tiles // 2 + 1,),
            out_shape=jax.ShapeDtypeStruct((tokens, d_model), BF16),
            in_specs=[
                pl.BlockSpec((tokens, 2 * TILE), lambda i: (0, jnp.minimum(i, last))),
                pl.BlockSpec((tokens, 2 * TILE), lambda i: (0, jnp.minimum(i, last) + tiles // 2)),
                pl.BlockSpec(((segs - 1) * STATE, 2 * TILE), lambda i: (0, jnp.minimum(i, last))),
                pl.BlockSpec((STATE, 2 * TILE), lambda i: (0, jnp.minimum(i, last))),
                fixed((tokens, 2 * STATE)), fixed((tokens, heads)),
                fixed((segs * heads, SEG)), fixed((8, heads)), fixed((1, heads)),
                any_space, any_space,
            ],
            out_specs=any_space,
            scratch_shapes=[
                pltpu.VMEM((tokens, d_model), F32),
                pltpu.VMEM((tokens, TILE), BF16),
                pltpu.VMEM((tokens, TILE), BF16),
                pltpu.VMEM((tokens, SEG), F32),
                pltpu.VMEM((4, TILE, d_model), BF16),
                pltpu.VMEM((tokens, d_model), BF16),
                pltpu.SemaphoreType.DMA((4,)),
                pltpu.SemaphoreType.DMA(()),
                pltpu.SemaphoreType.DMA((d_model // (2 * TILE),)),
            ],
            compiler_params=pltpu.CompilerParams(
                dimension_semantics=("arbitrary",), vmem_limit_bytes=62 * 1024 * 1024),
            cost_estimate=pl.CostEstimate(flops=2 * tokens * d_model * inner,
                                          bytes_accessed=2 * w_out.size, transcendentals=0),
            name="mix",
        )(u, u, loc, h_in, bc, gl, qt, dec, d_skip.reshape(1, heads), w_out, x_loc)

    return jax.shard_map(local_mixer, mesh=mesh, in_specs=(row_spec, P(), P(), P(), P(), P()),
                         out_specs=row_spec, check_vma=False)
```

```python
import jax
import jax.numpy as jnp
from jax import lax
from jax.experimental import pallas as pl
from jax.experimental.pallas import tpu as pltpu
from jax.sharding import PartitionSpec as P

SEG = 128
HEAD_DIM = 64
STATE = 128
TILE = 512
HALF = TILE // 2
TILE_HEADS = TILE // HEAD_DIM
LANES = 128
CHUNKS = 4
LAG_X = 9
LAG_Y = 14
LOG2E = 1.4426950408889634
MESH = pl.DeviceIdType.MESH
BF16 = jnp.bfloat16
F32 = jnp.float32


def dot32(a, b):
    return jnp.dot(a, b, preferred_element_type=F32)


def spread(v, pairs):
    rows = v.shape[0]
    low = lax.broadcasted_iota(jnp.int32, (rows, LANES), 1) < HEAD_DIM
    parts = []
    for p in range(pairs):
        left = jnp.broadcast_to(v[:, 2 * p:2 * p + 1], (rows, LANES))
        right = jnp.broadcast_to(v[:, 2 * p + 1:2 * p + 2], (rows, LANES))
        parts.append(jnp.where(low, left, right))
    return jnp.concatenate(parts, axis=1)


def lane_shift(v, first):
    return pltpu.roll(v, lax.rem(LANES - first, LANES), 1)


def project_kernel(x_hbm, w_hbm, an_hbm, db_hbm,
                   u_ref, loc_ref, hin_ref, bc_hbm, gl_hbm, qt_hbm, dec_hbm,
                   x_ref, wring, wdt_ref, an_ref, db_ref, bc_ref, gl_ref, qt_ref, dec_ref, isem, wsem, osem,
                   bt_ref, seg_dec, xw_ref, wst, uprev, drow, lsend, lall, s_own, rc, sx, rx, sy, ry, rf,
                   lsem, lrem, csem, crem, xsem, xrem, ysem, yrem, fsem, frem):
    step = pl.program_id(0)
    me = lax.axis_index("sp")
    tokens = x_ref.shape[0]
    segs = tokens // SEG
    tiles = s_own.shape[0]
    heads_at = 2 * tiles * TILE
    depth = x_ref.shape[1] // CHUNKS
    slots = wring.shape[0]
    small_loads = [
        pltpu.make_async_copy(db_hbm, db_ref, isem.at[0]),
        pltpu.make_async_copy(an_hbm, an_ref, isem.at[1]),
    ]

    def chunk_loads(q):
        part = slice(q * depth, (q + 1) * depth)
        return (pltpu.make_async_copy(x_hbm.at[:, part], x_ref.at[:, part], isem.at[2 + 2 * q]),
                pltpu.make_async_copy(w_hbm.at[part, heads_at:], wdt_ref.at[part, :], isem.at[3 + 2 * q]))

    def w_copy(at_step):
        slot = lax.rem(at_step, slots)
        first = pl.multiple_of(lax.rem(at_step + tiles, 2 * tiles) * TILE, TILE)
        return pltpu.make_async_copy(w_hbm.at[:, pl.ds(first, TILE)], wring.at[slot], wsem.at[slot])

    stores = [
        pltpu.make_async_copy(bc_ref, bc_hbm, osem.at[0]),
        pltpu.make_async_copy(gl_ref, gl_hbm, osem.at[1]),
        pltpu.make_async_copy(qt_ref, qt_hbm, osem.at[2]),
        pltpu.make_async_copy(dec_ref, dec_hbm, osem.at[3]),
    ]
    core = lax.rem(me, 2)
    xpos = lax.rem(me // 2, 2)
    ypos = me // 4
    peer_core = me + 1 - 2 * core
    peer_x = me + 2 - 4 * xpos
    peer_y = me + 4 - 8 * ypos
    barrier = pltpu.get_barrier_semaphore()

    def other(k):
        return lax.rem(me + k, 8)

    def log_copy(k):
        return pltpu.make_async_remote_copy(
            src_ref=lsend, dst_ref=lall.at[me], send_sem=lsem.at[k - 1], recv_sem=lrem.at[me],
            device_id={"sp": other(k)}, device_id_type=MESH)

    def remote(src, dst, send, recv, target):
        return pltpu.make_async_remote_copy(
            src_ref=src, dst_ref=dst, send_sem=send, recv_sem=recv,
            device_id={"sp": target}, device_id_type=MESH)

    def core_copy(c):
        return remote(s_own.at[c, 1 - core], rc.at[c], csem.at[c], crem.at[c], peer_core)

    def x_copy(c):
        return remote(sx.at[c], rx.at[c], xsem.at[c], xrem.at[c], peer_x)

    def y_copy(c):
        return remote(sy.at[c], ry.at[c], ysem.at[c], yrem.at[c], peer_y)

    def final_copy(c):
        return remote(sy.at[c], rf.at[c], fsem.at[c], frem.at[c], peer_core)

    def at_lag(lag):
        return jnp.logical_and(step >= lag, step < tiles + lag)

    def weigh(tile):
        weights = lane_shift(wst[...], tile * TILE_HEADS)
        for c in range(segs):
            rows = slice(c * SEG, (c + 1) * SEG)
            spread_rows = spread(weights[rows], TILE_HEADS // 2)
            xw_ref[rows, :] = (uprev[rows, :].astype(F32) * spread_rows).astype(BF16)

    def states(tile):
        dec = spread(lane_shift(seg_dec[...], tile * TILE_HEADS), TILE_HEADS // 2)
        state = dot32(bt_ref[:SEG, :], xw_ref[:SEG, :])
        for c in range(1, segs):
            rows = slice(c * SEG, (c + 1) * SEG)
            loc_ref[(c - 1) * STATE:c * STATE, :] = state
            state = dec[c:c + 1] * state + dot32(bt_ref[rows, :], xw_ref[rows, :])
        s_own[tile, 0] = state[:, :HALF]
        s_own[tile, 1] = state[:, HALF:]

    def project(keep):
        u = dot32(x_ref[...], wring[lax.rem(step, slots)]).astype(BF16)
        u_ref[...] = u
        if keep:
            uprev[...] = u

    @pl.when(step == 0)
    def _():
        for k in range(1, 8):
            pl.semaphore_signal(barrier, inc=1, device_id={"sp": other(k)}, device_id_type=MESH)
        for q in range(CHUNKS):
            for load in chunk_loads(q):
                load.start()
        for load in small_loads:
            load.start()
        for k in range(slots):
            w_copy(k).start()
        for load in small_loads:
            load.wait()
        last_columns = None
        for q in range(CHUNKS):
            for load in chunk_loads(q):
                load.wait()
            part = slice(q * depth, (q + 1) * depth)
            term = dot32(x_ref[:, part], wdt_ref[part, :])
            last_columns = term if last_columns is None else last_columns + term
        last_columns = last_columns.astype(BF16)
        bc = last_columns[:, :2 * STATE]
        bc_ref[...] = bc
        raw = last_columns[:, 2 * STATE:].astype(F32) + db_ref[...]
        dt = jnp.maximum(raw, 0.0) + jnp.log1p(jnp.exp(-jnp.abs(raw)))
        logs = dt * an_ref[...]
        tri = (lax.broadcasted_iota(jnp.int32, (SEG, SEG), 0)
               >= lax.broadcasted_iota(jnp.int32, (SEG, SEG), 1)).astype(F32)
        total = jnp.zeros((1, LANES), F32)
        row = lax.broadcasted_iota(jnp.int32, (8, LANES), 0)
        dec = jnp.zeros((8, LANES), F32)
        before = jnp.zeros((8, LANES), F32)
        for c in range(segs):
            rows = slice(c * SEG, (c + 1) * SEG)
            cum = jnp.dot(tri, logs[rows], precision=lax.Precision.HIGHEST, preferred_element_type=F32)
            last = cum[SEG - 1:SEG]
            wst[rows, :] = jnp.exp(last - cum) * dt[rows]
            gl_ref[rows, :] = cum * LOG2E
            qt_ref[rows, :] = jnp.transpose(cum * LOG2E - jnp.log2(dt[rows]))
            bt_ref[rows, :] = jnp.transpose(bc[rows, :STATE].astype(F32)).astype(BF16)
            dec = jnp.where(row == c, jnp.exp(last), dec)
            before = jnp.where(row == c, jnp.exp(total), before)
            total = total + last
        seg_dec[...] = dec
        dec_ref[...] = before
        lsend[...] = jnp.broadcast_to(total, (8, LANES))

    def s_of(mine, c):
        return jnp.where(mine, s_own[c, core], rc[c])

    @pl.when(step == 2)
    def _():
        pl.semaphore_wait(barrier, 7)
        for store in stores:
            store.start()
        for k in range(1, 8):
            log_copy(k).start()
        lall[me] = lsend[...]

    @pl.when(jnp.logical_and(step >= 3, step < tiles + 5))
    def _():
        @pl.when(at_lag(3))
        def _():
            core_copy(step - 3).start()

        @pl.when(step == 4)
        def _():
            for k in range(1, 8):
                log_copy(k).wait_send()
                source = other(k)
                pltpu.make_async_remote_copy(
                    src_ref=lsend, dst_ref=lall.at[source], send_sem=lsem.at[k - 1], recv_sem=lrem.at[source],
                    device_id={"sp": source}, device_id_type=MESH).wait_recv()
            chip = ypos * 4
            row = lax.broadcasted_iota(jnp.int32, (8, LANES), 0)
            logs = jnp.where(row == 0, lall[me - core + 1], 0.0)
            logs = jnp.where(row == 1, lall[chip + 2] + lall[chip + 3], logs)
            logs = jnp.where(jnp.logical_and(row == 2, xpos == 1), lall[chip] + lall[chip + 1], logs)
            logs = jnp.where(row == 3, lall[me - core], logs)
            decays = jnp.exp(logs)
            for c in range(tiles):
                drow[c] = spread(lane_shift(decays, c * TILE_HEADS + core * (TILE_HEADS // 2)), 2)

        @pl.when(at_lag(4))
        def _():
            c = step - 4
            core_copy(c).wait()
            sx[c] = drow[c, 0:1] * s_of(core == 0, c) + s_of(core == 1, c)

        @pl.when(at_lag(5))
        def _():
            x_copy(step - 5).start()

    @pl.when(jnp.logical_and(step >= LAG_X, step < tiles + LAG_X + 1))
    def _():
        @pl.when(at_lag(LAG_X))
        def _():
            c = step - LAG_X
            x_copy(c).wait()
            mine, got = sx[c], rx[c]
            early = jnp.where(xpos == 0, mine, got)
            late = jnp.where(xpos == 0, got, mine)
            sy[c] = drow[c, 1:2] * early + late

        @pl.when(at_lag(LAG_X + 1))
        def _():
            y_copy(step - LAG_X - 1).start()

    @pl.when(step >= LAG_Y)
    def _():
        @pl.when(at_lag(LAG_Y))
        def _():
            c = step - LAG_Y
            y_copy(c).wait()
            before = jnp.where(xpos == 1, rx[c], 0.0) + jnp.where(ypos == 1, drow[c, 2:3] * ry[c], 0.0)
            after = drow[c, 3:4] * before + s_of(core == 0, c)
            sx[c] = jnp.where(core == 0, before, after)
            sy[c] = jnp.where(core == 0, after, before)

        @pl.when(at_lag(LAG_Y + 1))
        def _():
            final_copy(step - LAG_Y - 1).start()

        @pl.when(at_lag(LAG_Y + 2))
        def _():
            c = step - LAG_Y - 2
            final_copy(c).wait()
            mine, got = sx[c], rf[c]
            hin_ref[:, :HALF] = jnp.where(core == 0, mine, got)
            hin_ref[:, HALF:] = jnp.where(core == 0, got, mine)

    with_state = jnp.logical_and(step >= 1, step <= tiles + 1)

    @pl.when(with_state)
    def _():
        w_copy(step).wait()
        states(jnp.maximum(step - 2, 0))
        weigh(step - 1)
        project(True)

    @pl.when(step == 0)
    def _():
        w_copy(step).wait()
        project(True)

    @pl.when(step > tiles + 1)
    def _():
        w_copy(step).wait()
        project(False)

    @pl.when(step + slots < 2 * tiles)
    def _():
        w_copy(step + slots).start()

    @pl.when(step == 2 * tiles - 1)
    def _():
        for store in stores:
            store.wait()


def mix_kernel(z_ref, xs_ref, loc_ref, h_ref, bc_ref, gl_ref, qt_ref, dec_ref, ds_ref, w_hbm, x_hbm,
               out_hbm, acc, gated_a, gated_b, scores, wbuf, out_ref, w_sem, x_sem, o_sem):
    step = pl.program_id(0)
    steps = pl.num_programs(0)
    tokens, d_model = acc.shape
    segs = tokens // SEG
    slots = wbuf.shape[0]
    groups = w_hbm.shape[0] // TILE
    x_copy = pltpu.make_async_copy(x_hbm, out_ref, x_sem)

    def w_copy(group):
        slot = lax.rem(group, slots)
        first = pl.multiple_of(group * TILE, TILE)
        return pltpu.make_async_copy(w_hbm.at[pl.ds(first, TILE), :], wbuf.at[slot], w_sem.at[slot])

    def w_next(group):
        @pl.when(group + slots < groups)
        def _():
            w_copy(group + slots).start()

    def dot_slice(k, source, group):
        cols = slice(k * HALF, (k + 1) * HALF)
        acc[:, cols] += dot32(source[...], wbuf[lax.rem(group, slots), :, cols])

    def group_outputs(half, target, big):
        base = half * TILE
        first = (2 * step + half) * TILE_HEADS
        gl = lane_shift(gl_ref[...], first)
        dec = spread(lane_shift(dec_ref[...], first), TILE_HEADS // 2)
        skip = spread(lane_shift(jnp.broadcast_to(ds_ref[...], (8, LANES)), first), TILE_HEADS // 2)[:1]
        causal = (lax.broadcasted_iota(jnp.int32, (SEG, SEG), 0)
                  >= lax.broadcasted_iota(jnp.int32, (SEG, SEG), 1))
        low = lax.broadcasted_iota(jnp.int32, (SEG, LANES), 1) < HEAD_DIM
        zero = jnp.zeros((SEG, LANES), BF16)
        waiting = []
        unit = 0
        for c in range(segs):
            rows = slice(c * SEG, (c + 1) * SEG)
            state = h_ref[:, base:base + TILE]
            if c > 0:
                state = dec[c:c + 1] * state + loc_ref[(c - 1) * STATE:c * STATE, base:base + TILE]
            y_state = dot32(bc_ref[rows, STATE:], state.astype(BF16))
            q_rows = qt_ref[pl.ds(pl.multiple_of(c * SEG + first, TILE_HEADS), TILE_HEADS), :]
            for p in range(TILE_HEADS // 2):
                cols = slice(base + p * LANES, base + (p + 1) * LANES)
                sc = scores[rows, :]
                col_a = jnp.broadcast_to(gl[rows, 2 * p:2 * p + 1], (SEG, LANES))
                col_b = jnp.broadcast_to(gl[rows, 2 * p + 1:2 * p + 2], (SEG, LANES))
                g_a = jnp.where(causal, sc * jnp.exp2(col_a - q_rows[2 * p:2 * p + 1]), 0.0).astype(BF16)
                g_b = jnp.where(causal, sc * jnp.exp2(col_b - q_rows[2 * p + 1:2 * p + 2]), 0.0).astype(BF16)
                xp = xs_ref[rows, cols]
                rhs = jnp.concatenate([jnp.where(low, xp, zero), jnp.where(low, zero, xp)], axis=0)
                if big is not None:
                    dot_slice(unit, *big)
                y = dot32(jnp.concatenate([g_a, g_b], axis=1), rhs)
                if len(waiting) == 2:
                    waiting.pop(0)()

                def pending(y=y, rows=rows, cols=cols, p=p, y_state=y_state, col_a=col_a, col_b=col_b):
                    here = slice(p * LANES, (p + 1) * LANES)
                    total = y + y_state[:, here] * jnp.exp2(jnp.where(low, col_a, col_b))
                    total = total + skip[:, here] * xs_ref[rows, cols].astype(F32)
                    z = z_ref[rows, cols].astype(F32)
                    target[rows, here] = (total * (z / (1.0 + jnp.exp(-z)))).astype(BF16)
                waiting.append(pending)
                unit += 1
        for pending in waiting:
            pending()

    @pl.when(step == 0)
    def _():
        for group in range(slots):
            w_copy(group).start()
        x_copy.start()
        acc[...] = jnp.zeros_like(acc)
        for c in range(segs):
            rows = slice(c * SEG, (c + 1) * SEG)
            scores[rows, :] = lax.dot_general(bc_ref[rows, STATE:], bc_ref[rows, :STATE],
                                              (((1,), (1,)), ((), ())), preferred_element_type=F32)
        group_outputs(0, gated_a, None)
        w_copy(0).wait()
        group_outputs(1, gated_b, (gated_a, 0))
        w_next(0)

    @pl.when(jnp.logical_and(step > 0, step < steps - 1))
    def _():
        w_copy(2 * step - 1).wait()
        w_copy(2 * step).wait()
        group_outputs(0, gated_a, (gated_b, 2 * step - 1))
        group_outputs(1, gated_b, (gated_a, 2 * step))
        w_next(2 * step - 1)
        w_next(2 * step)

    @pl.when(step == steps - 1)
    def _():
        x_copy.wait()
        w_copy(groups - 1).wait()
        copies = []
        for k in range(d_model // (2 * TILE)):
            cols = slice(2 * k * TILE, 2 * (k + 1) * TILE)
            total = acc[:, cols] + dot32(gated_b[...], wbuf[(groups - 1) % slots, :, cols])
            out_ref[:, cols] = (out_ref[:, cols].astype(F32) + total).astype(BF16)
            copies.append(pltpu.make_async_copy(out_ref.at[:, cols], out_hbm.at[:, cols], o_sem.at[k]))
            copies[-1].start()
        for copy in copies:
            copy.wait()


def solution(mesh):
    row_spec = P(("dp", "sp"), None)

    def local_mixer(x_loc, w_in, a_neg, dt_bias, d_skip, w_out):
        tokens, d_model = x_loc.shape
        inner = w_out.shape[0]
        heads = a_neg.shape[0]
        tiles = inner // TILE
        segs = tokens // SEG
        assert mesh.shape["sp"] == 8 and heads == LANES and inner == heads * HEAD_DIM
        assert tiles >= LAG_Y + 2
        def fixed(shape):
            return pl.BlockSpec(shape, lambda i: (0,) * len(shape), pipeline_mode=pl.Buffered(1))

        half = (tiles, STATE, HALF)
        sems = pltpu.SemaphoreType.DMA((tiles,))
        any_space = pl.BlockSpec(memory_space=pl.ANY)
        u, loc, h_in, bc, gl, qt, dec = pl.pallas_call(
            project_kernel,
            grid=(2 * tiles,),
            out_shape=[
                jax.ShapeDtypeStruct((tokens, 2 * inner), BF16),
                jax.ShapeDtypeStruct(((segs - 1) * STATE, inner), F32),
                jax.ShapeDtypeStruct((STATE, inner), F32),
                jax.ShapeDtypeStruct((tokens, 2 * STATE), BF16),
                jax.ShapeDtypeStruct((tokens, heads), F32),
                jax.ShapeDtypeStruct((segs * heads, SEG), F32),
                jax.ShapeDtypeStruct((8, heads), F32),
            ],
            in_specs=[
                any_space, any_space, any_space, any_space,
            ],
            out_specs=[
                pl.BlockSpec((tokens, TILE), lambda i: (0, lax.rem(i + tiles, 2 * tiles))),
                pl.BlockSpec(((segs - 1) * STATE, TILE), lambda i: (0, jnp.clip(i - 2, 0, tiles - 1))),
                pl.BlockSpec((STATE, TILE), lambda i: (0, jnp.maximum(i - (LAG_Y + 2), 0))),
                any_space, any_space, any_space, any_space,
            ],
            scratch_shapes=[
                pltpu.VMEM((tokens, d_model), BF16),
                pltpu.VMEM((3, d_model, TILE), BF16),
                pltpu.VMEM((d_model, 2 * STATE + heads), BF16),
                pltpu.VMEM((1, heads), F32), pltpu.VMEM((1, heads), F32),
                pltpu.VMEM((tokens, 2 * STATE), BF16),
                pltpu.VMEM((tokens, heads), F32),
                pltpu.VMEM((segs * heads, SEG), F32),
                pltpu.VMEM((8, heads), F32),
                pltpu.SemaphoreType.DMA((2 + 2 * CHUNKS,)), pltpu.SemaphoreType.DMA((3,)), pltpu.SemaphoreType.DMA((4,)),
                pltpu.VMEM((segs * STATE, SEG), BF16),
                pltpu.VMEM((8, heads), F32),
                pltpu.VMEM((tokens, TILE), BF16),
                pltpu.VMEM((tokens, heads), F32),
                pltpu.VMEM((tokens, TILE), BF16),
                pltpu.VMEM((tiles, 8, HALF), F32),
                pltpu.VMEM((8, heads), F32),
                pltpu.VMEM((8, 8, heads), F32),
                pltpu.VMEM((tiles, 2, STATE, HALF), F32),
                pltpu.VMEM(half, F32), pltpu.VMEM(half, F32), pltpu.VMEM(half, F32),
                pltpu.VMEM(half, F32), pltpu.VMEM(half, F32), pltpu.VMEM(half, F32),
                pltpu.SemaphoreType.DMA((7,)), pltpu.SemaphoreType.DMA((8,)),
                sems, sems, sems, sems, sems, sems, sems, sems,
            ],
            compiler_params=pltpu.CompilerParams(
                dimension_semantics=("arbitrary",), collective_id=0, has_side_effects=True,
                vmem_limit_bytes=60 * 1024 * 1024),
            cost_estimate=pl.CostEstimate(flops=2 * tokens * d_model * w_in.shape[1],
                                          bytes_accessed=2 * w_in.size, transcendentals=0),
            name="project",
        )(x_loc, w_in, a_neg.reshape(1, heads), dt_bias.reshape(1, heads))

        last = tiles // 2 - 1
        return pl.pallas_call(
            mix_kernel,
            grid=(tiles // 2 + 1,),
            out_shape=jax.ShapeDtypeStruct((tokens, d_model), BF16),
            in_specs=[
                pl.BlockSpec((tokens, 2 * TILE), lambda i: (0, jnp.minimum(i, last))),
                pl.BlockSpec((tokens, 2 * TILE), lambda i: (0, jnp.minimum(i, last) + tiles // 2)),
                pl.BlockSpec(((segs - 1) * STATE, 2 * TILE), lambda i: (0, jnp.minimum(i, last))),
                pl.BlockSpec((STATE, 2 * TILE), lambda i: (0, jnp.minimum(i, last))),
                fixed((tokens, 2 * STATE)), fixed((tokens, heads)),
                fixed((segs * heads, SEG)), fixed((8, heads)), fixed((1, heads)),
                any_space, any_space,
            ],
            out_specs=any_space,
            scratch_shapes=[
                pltpu.VMEM((tokens, d_model), F32),
                pltpu.VMEM((tokens, TILE), BF16),
                pltpu.VMEM((tokens, TILE), BF16),
                pltpu.VMEM((tokens, SEG), F32),
                pltpu.VMEM((4, TILE, d_model), BF16),
                pltpu.VMEM((tokens, d_model), BF16),
                pltpu.SemaphoreType.DMA((4,)),
                pltpu.SemaphoreType.DMA(()),
                pltpu.SemaphoreType.DMA((d_model // (2 * TILE),)),
            ],
            compiler_params=pltpu.CompilerParams(
                dimension_semantics=("arbitrary",), vmem_limit_bytes=62 * 1024 * 1024),
            cost_estimate=pl.CostEstimate(flops=2 * tokens * d_model * inner,
                                          bytes_accessed=2 * w_out.size, transcendentals=0),
            name="mix",
        )(u, u, loc, h_in, bc, gl, qt, dec, d_skip.reshape(1, heads), w_out, x_loc)

    return jax.shard_map(local_mixer, mesh=mesh, in_specs=(row_spec, P(), P(), P(), P(), P()),
                         out_specs=row_spec, check_vma=False)
```

```python
import jax
import jax.numpy as jnp
from jax import lax
from jax.experimental import pallas as pl
from jax.experimental.pallas import tpu as pltpu
from jax.sharding import PartitionSpec as P

SEG = 128
HEAD_DIM = 64
STATE = 128
TILE = 512
HALF = TILE // 2
TILE_HEADS = TILE // HEAD_DIM
LANES = 128
CHUNKS = 2
LAG_X = 9
LAG_Y = 14
LOG2E = 1.4426950408889634
MESH = pl.DeviceIdType.MESH
BF16 = jnp.bfloat16
F32 = jnp.float32


def dot32(a, b):
    return jnp.dot(a, b, preferred_element_type=F32)


def spread(v, pairs):
    rows = v.shape[0]
    low = lax.broadcasted_iota(jnp.int32, (rows, LANES), 1) < HEAD_DIM
    parts = []
    for p in range(pairs):
        left = jnp.broadcast_to(v[:, 2 * p:2 * p + 1], (rows, LANES))
        right = jnp.broadcast_to(v[:, 2 * p + 1:2 * p + 2], (rows, LANES))
        parts.append(jnp.where(low, left, right))
    return jnp.concatenate(parts, axis=1)


def lane_shift(v, first):
    return pltpu.roll(v, lax.rem(LANES - first, LANES), 1)


def project_kernel(x_hbm, w_hbm, an_hbm, db_hbm,
                   u_ref, loc_ref, hin_ref, bc_hbm, gl_hbm, qt_hbm, dec_hbm,
                   x_ref, wring, wdt_ref, an_ref, db_ref, bc_ref, gl_ref, qt_ref, dec_ref, isem, wsem, osem,
                   bt_ref, seg_dec, xw_ref, wst, uprev, drow, lsend, lall, s_own, rc, sx, rx, sy, ry, rf,
                   lsem, lrem, csem, crem, xsem, xrem, ysem, yrem, fsem, frem):
    step = pl.program_id(0)
    me = lax.axis_index("sp")
    tokens = x_ref.shape[0]
    segs = tokens // SEG
    tiles = s_own.shape[0]
    heads_at = 2 * tiles * TILE
    depth = x_ref.shape[1] // CHUNKS
    slots = wring.shape[0]
    small_loads = [
        pltpu.make_async_copy(db_hbm, db_ref, isem.at[0]),
        pltpu.make_async_copy(an_hbm, an_ref, isem.at[1]),
    ]

    def chunk_loads(q):
        part = slice(q * depth, (q + 1) * depth)
        return (pltpu.make_async_copy(x_hbm.at[:, part], x_ref.at[:, part], isem.at[2 + 2 * q]),
                pltpu.make_async_copy(w_hbm.at[part, heads_at:], wdt_ref.at[part, :], isem.at[3 + 2 * q]))

    def w_copy(at_step):
        slot = lax.rem(at_step, slots)
        first = pl.multiple_of(lax.rem(at_step + tiles, 2 * tiles) * TILE, TILE)
        return pltpu.make_async_copy(w_hbm.at[:, pl.ds(first, TILE)], wring.at[slot], wsem.at[slot])

    stores = [
        pltpu.make_async_copy(bc_ref, bc_hbm, osem.at[0]),
        pltpu.make_async_copy(gl_ref, gl_hbm, osem.at[1]),
        pltpu.make_async_copy(qt_ref, qt_hbm, osem.at[2]),
        pltpu.make_async_copy(dec_ref, dec_hbm, osem.at[3]),
    ]
    core = lax.rem(me, 2)
    xpos = lax.rem(me // 2, 2)
    ypos = me // 4
    peer_core = me + 1 - 2 * core
    peer_x = me + 2 - 4 * xpos
    peer_y = me + 4 - 8 * ypos
    barrier = pltpu.get_barrier_semaphore()

    def other(k):
        return lax.rem(me + k, 8)

    def log_copy(k):
        return pltpu.make_async_remote_copy(
            src_ref=lsend, dst_ref=lall.at[me], send_sem=lsem.at[k - 1], recv_sem=lrem.at[me],
            device_id={"sp": other(k)}, device_id_type=MESH)

    def remote(src, dst, send, recv, target):
        return pltpu.make_async_remote_copy(
            src_ref=src, dst_ref=dst, send_sem=send, recv_sem=recv,
            device_id={"sp": target}, device_id_type=MESH)

    def core_copy(c):
        return remote(s_own.at[c, 1 - core], rc.at[c], csem.at[c], crem.at[c], peer_core)

    def x_copy(c):
        return remote(sx.at[c], rx.at[c], xsem.at[c], xrem.at[c], peer_x)

    def y_copy(c):
        return remote(sy.at[c], ry.at[c], ysem.at[c], yrem.at[c], peer_y)

    def final_copy(c):
        return remote(sy.at[c], rf.at[c], fsem.at[c], frem.at[c], peer_core)

    def at_lag(lag):
        return jnp.logical_and(step >= lag, step < tiles + lag)

    def weigh(tile):
        weights = lane_shift(wst[...], tile * TILE_HEADS)
        for c in range(segs):
            rows = slice(c * SEG, (c + 1) * SEG)
            spread_rows = spread(weights[rows], TILE_HEADS // 2)
            xw_ref[rows, :] = (uprev[rows, :].astype(F32) * spread_rows).astype(BF16)

    def states(tile):
        dec = spread(lane_shift(seg_dec[...], tile * TILE_HEADS), TILE_HEADS // 2)
        state = dot32(bt_ref[:SEG, :], xw_ref[:SEG, :])
        for c in range(1, segs):
            rows = slice(c * SEG, (c + 1) * SEG)
            loc_ref[(c - 1) * STATE:c * STATE, :] = state
            state = dec[c:c + 1] * state + dot32(bt_ref[rows, :], xw_ref[rows, :])
        s_own[tile, 0] = state[:, :HALF]
        s_own[tile, 1] = state[:, HALF:]

    def project(keep):
        u = dot32(x_ref[...], wring[lax.rem(step, slots)]).astype(BF16)
        u_ref[...] = u
        if keep:
            uprev[...] = u

    @pl.when(step == 0)
    def _():
        for k in range(1, 8):
            pl.semaphore_signal(barrier, inc=1, device_id={"sp": other(k)}, device_id_type=MESH)
        for q in range(CHUNKS):
            for load in chunk_loads(q):
                load.start()
        for load in small_loads:
            load.start()
        for k in range(slots):
            w_copy(k).start()
        for load in small_loads:
            load.wait()
        last_columns = None
        for q in range(CHUNKS):
            for load in chunk_loads(q):
                load.wait()
            part = slice(q * depth, (q + 1) * depth)
            term = dot32(x_ref[:, part], wdt_ref[part, :])
            last_columns = term if last_columns is None else last_columns + term
        last_columns = last_columns.astype(BF16)
        bc = last_columns[:, :2 * STATE]
        bc_ref[...] = bc
        raw = last_columns[:, 2 * STATE:].astype(F32) + db_ref[...]
        dt = jnp.maximum(raw, 0.0) + jnp.log1p(jnp.exp(-jnp.abs(raw)))
        logs = dt * an_ref[...]
        tri = (lax.broadcasted_iota(jnp.int32, (SEG, SEG), 0)
               >= lax.broadcasted_iota(jnp.int32, (SEG, SEG), 1)).astype(F32)
        total = jnp.zeros((1, LANES), F32)
        row = lax.broadcasted_iota(jnp.int32, (8, LANES), 0)
        dec = jnp.zeros((8, LANES), F32)
        before = jnp.zeros((8, LANES), F32)
        for c in range(segs):
            rows = slice(c * SEG, (c + 1) * SEG)
            cum = jnp.dot(tri, logs[rows], precision=lax.Precision.HIGHEST, preferred_element_type=F32)
            last = cum[SEG - 1:SEG]
            wst[rows, :] = jnp.exp(last - cum) * dt[rows]
            gl_ref[rows, :] = cum * LOG2E
            qt_ref[rows, :] = jnp.transpose(cum * LOG2E - jnp.log2(dt[rows]))
            bt_ref[rows, :] = jnp.transpose(bc[rows, :STATE].astype(F32)).astype(BF16)
            dec = jnp.where(row == c, jnp.exp(last), dec)
            before = jnp.where(row == c, jnp.exp(total), before)
            total = total + last
        seg_dec[...] = dec
        dec_ref[...] = before
        lsend[...] = jnp.broadcast_to(total, (8, LANES))

    def s_of(mine, c):
        return jnp.where(mine, s_own[c, core], rc[c])

    @pl.when(step == 2)
    def _():
        pl.semaphore_wait(barrier, 7)
        for store in stores:
            store.start()
        for k in range(1, 8):
            log_copy(k).start()
        lall[me] = lsend[...]

    @pl.when(jnp.logical_and(step >= 3, step < tiles + 5))
    def _():
        @pl.when(at_lag(3))
        def _():
            core_copy(step - 3).start()

        @pl.when(step == 4)
        def _():
            for k in range(1, 8):
                log_copy(k).wait_send()
                source = other(k)
                pltpu.make_async_remote_copy(
                    src_ref=lsend, dst_ref=lall.at[source], send_sem=lsem.at[k - 1], recv_sem=lrem.at[source],
                    device_id={"sp": source}, device_id_type=MESH).wait_recv()
            chip = ypos * 4
            row = lax.broadcasted_iota(jnp.int32, (8, LANES), 0)
            logs = jnp.where(row == 0, lall[me - core + 1], 0.0)
            logs = jnp.where(row == 1, lall[chip + 2] + lall[chip + 3], logs)
            logs = jnp.where(jnp.logical_and(row == 2, xpos == 1), lall[chip] + lall[chip + 1], logs)
            logs = jnp.where(row == 3, lall[me - core], logs)
            decays = jnp.exp(logs)
            for c in range(tiles):
                drow[c] = spread(lane_shift(decays, c * TILE_HEADS + core * (TILE_HEADS // 2)), 2)

        @pl.when(at_lag(4))
        def _():
            c = step - 4
            core_copy(c).wait()
            sx[c] = drow[c, 0:1] * s_of(core == 0, c) + s_of(core == 1, c)

        @pl.when(at_lag(5))
        def _():
            x_copy(step - 5).start()

    @pl.when(jnp.logical_and(step >= LAG_X, step < tiles + LAG_X + 1))
    def _():
        @pl.when(at_lag(LAG_X))
        def _():
            c = step - LAG_X
            x_copy(c).wait()
            mine, got = sx[c], rx[c]
            early = jnp.where(xpos == 0, mine, got)
            late = jnp.where(xpos == 0, got, mine)
            sy[c] = drow[c, 1:2] * early + late

        @pl.when(at_lag(LAG_X + 1))
        def _():
            y_copy(step - LAG_X - 1).start()

    @pl.when(step >= LAG_Y)
    def _():
        @pl.when(at_lag(LAG_Y))
        def _():
            c = step - LAG_Y
            y_copy(c).wait()
            before = jnp.where(xpos == 1, rx[c], 0.0) + jnp.where(ypos == 1, drow[c, 2:3] * ry[c], 0.0)
            after = drow[c, 3:4] * before + s_of(core == 0, c)
            sx[c] = jnp.where(core == 0, before, after)
            sy[c] = jnp.where(core == 0, after, before)

        @pl.when(at_lag(LAG_Y + 1))
        def _():
            final_copy(step - LAG_Y - 1).start()

        @pl.when(at_lag(LAG_Y + 2))
        def _():
            c = step - LAG_Y - 2
            final_copy(c).wait()
            mine, got = sx[c], rf[c]
            hin_ref[:, :HALF] = jnp.where(core == 0, mine, got)
            hin_ref[:, HALF:] = jnp.where(core == 0, got, mine)

    with_state = jnp.logical_and(step >= 1, step <= tiles + 1)

    @pl.when(with_state)
    def _():
        w_copy(step).wait()
        states(jnp.maximum(step - 2, 0))
        weigh(step - 1)
        project(True)

    @pl.when(step == 0)
    def _():
        w_copy(step).wait()
        project(True)

    @pl.when(step > tiles + 1)
    def _():
        w_copy(step).wait()
        project(False)

    @pl.when(step + slots < 2 * tiles)
    def _():
        w_copy(step + slots).start()

    @pl.when(step == 2 * tiles - 1)
    def _():
        for store in stores:
            store.wait()


def mix_kernel(z_ref, xs_ref, loc_ref, h_ref, bc_ref, gl_ref, qt_ref, dec_ref, ds_ref, w_hbm, x_hbm,
               out_hbm, acc, gated_a, gated_b, scores, wbuf, out_ref, w_sem, x_sem, o_sem):
    step = pl.program_id(0)
    steps = pl.num_programs(0)
    tokens, d_model = acc.shape
    segs = tokens // SEG
    slots = wbuf.shape[0]
    groups = w_hbm.shape[0] // TILE
    x_copy = pltpu.make_async_copy(x_hbm, out_ref, x_sem)

    def w_copy(group):
        slot = lax.rem(group, slots)
        first = pl.multiple_of(group * TILE, TILE)
        return pltpu.make_async_copy(w_hbm.at[pl.ds(first, TILE), :], wbuf.at[slot], w_sem.at[slot])

    def w_next(group):
        @pl.when(group + slots < groups)
        def _():
            w_copy(group + slots).start()

    def dot_slice(k, source, group):
        cols = slice(k * HALF, (k + 1) * HALF)
        acc[:, cols] += dot32(source[...], wbuf[lax.rem(group, slots), :, cols])

    def group_outputs(half, target, big):
        base = half * TILE
        first = (2 * step + half) * TILE_HEADS
        gl = lane_shift(gl_ref[...], first)
        dec = spread(lane_shift(dec_ref[...], first), TILE_HEADS // 2)
        skip = spread(lane_shift(jnp.broadcast_to(ds_ref[...], (8, LANES)), first), TILE_HEADS // 2)[:1]
        causal = (lax.broadcasted_iota(jnp.int32, (SEG, SEG), 0)
                  >= lax.broadcasted_iota(jnp.int32, (SEG, SEG), 1))
        low = lax.broadcasted_iota(jnp.int32, (SEG, LANES), 1) < HEAD_DIM
        zero = jnp.zeros((SEG, LANES), BF16)
        waiting = []
        unit = 0
        for c in range(segs):
            rows = slice(c * SEG, (c + 1) * SEG)
            state = h_ref[:, base:base + TILE]
            if c > 0:
                state = dec[c:c + 1] * state + loc_ref[(c - 1) * STATE:c * STATE, base:base + TILE]
            y_state = dot32(bc_ref[rows, STATE:], state.astype(BF16))
            q_rows = qt_ref[pl.ds(pl.multiple_of(c * SEG + first, TILE_HEADS), TILE_HEADS), :]
            for p in range(TILE_HEADS // 2):
                cols = slice(base + p * LANES, base + (p + 1) * LANES)
                sc = scores[rows, :]
                col_a = jnp.broadcast_to(gl[rows, 2 * p:2 * p + 1], (SEG, LANES))
                col_b = jnp.broadcast_to(gl[rows, 2 * p + 1:2 * p + 2], (SEG, LANES))
                g_a = jnp.where(causal, sc * jnp.exp2(col_a - q_rows[2 * p:2 * p + 1]), 0.0).astype(BF16)
                g_b = jnp.where(causal, sc * jnp.exp2(col_b - q_rows[2 * p + 1:2 * p + 2]), 0.0).astype(BF16)
                xp = xs_ref[rows, cols]
                rhs = jnp.concatenate([jnp.where(low, xp, zero), jnp.where(low, zero, xp)], axis=0)
                if big is not None:
                    dot_slice(unit, *big)
                y = dot32(jnp.concatenate([g_a, g_b], axis=1), rhs)
                if len(waiting) == 2:
                    waiting.pop(0)()

                def pending(y=y, rows=rows, cols=cols, p=p, y_state=y_state, col_a=col_a, col_b=col_b):
                    here = slice(p * LANES, (p + 1) * LANES)
                    total = y + y_state[:, here] * jnp.exp2(jnp.where(low, col_a, col_b))
                    total = total + skip[:, here] * xs_ref[rows, cols].astype(F32)
                    z = z_ref[rows, cols].astype(F32)
                    target[rows, here] = (total * (z / (1.0 + jnp.exp(-z)))).astype(BF16)
                waiting.append(pending)
                unit += 1
        for pending in waiting:
            pending()

    @pl.when(step == 0)
    def _():
        for group in range(slots):
            w_copy(group).start()
        x_copy.start()
        acc[...] = jnp.zeros_like(acc)
        for c in range(segs):
            rows = slice(c * SEG, (c + 1) * SEG)
            scores[rows, :] = lax.dot_general(bc_ref[rows, STATE:], bc_ref[rows, :STATE],
                                              (((1,), (1,)), ((), ())), preferred_element_type=F32)
        group_outputs(0, gated_a, None)
        w_copy(0).wait()
        group_outputs(1, gated_b, (gated_a, 0))
        w_next(0)

    @pl.when(jnp.logical_and(step > 0, step < steps - 1))
    def _():
        w_copy(2 * step - 1).wait()
        w_copy(2 * step).wait()
        group_outputs(0, gated_a, (gated_b, 2 * step - 1))
        group_outputs(1, gated_b, (gated_a, 2 * step))
        w_next(2 * step - 1)
        w_next(2 * step)

    @pl.when(step == steps - 1)
    def _():
        x_copy.wait()
        w_copy(groups - 1).wait()
        copies = []
        for k in range(d_model // (2 * TILE)):
            cols = slice(2 * k * TILE, 2 * (k + 1) * TILE)
            total = acc[:, cols] + dot32(gated_b[...], wbuf[(groups - 1) % slots, :, cols])
            out_ref[:, cols] = (out_ref[:, cols].astype(F32) + total).astype(BF16)
            copies.append(pltpu.make_async_copy(out_ref.at[:, cols], out_hbm.at[:, cols], o_sem.at[k]))
            copies[-1].start()
        for copy in copies:
            copy.wait()


def solution(mesh):
    row_spec = P(("dp", "sp"), None)

    def local_mixer(x_loc, w_in, a_neg, dt_bias, d_skip, w_out):
        tokens, d_model = x_loc.shape
        inner = w_out.shape[0]
        heads = a_neg.shape[0]
        tiles = inner // TILE
        segs = tokens // SEG
        assert mesh.shape["sp"] == 8 and heads == LANES and inner == heads * HEAD_DIM
        assert tiles >= LAG_Y + 2
        def fixed(shape):
            return pl.BlockSpec(shape, lambda i: (0,) * len(shape), pipeline_mode=pl.Buffered(1))

        half = (tiles, STATE, HALF)
        sems = pltpu.SemaphoreType.DMA((tiles,))
        any_space = pl.BlockSpec(memory_space=pl.ANY)
        u, loc, h_in, bc, gl, qt, dec = pl.pallas_call(
            project_kernel,
            grid=(2 * tiles,),
            out_shape=[
                jax.ShapeDtypeStruct((tokens, 2 * inner), BF16),
                jax.ShapeDtypeStruct(((segs - 1) * STATE, inner), F32),
                jax.ShapeDtypeStruct((STATE, inner), F32),
                jax.ShapeDtypeStruct((tokens, 2 * STATE), BF16),
                jax.ShapeDtypeStruct((tokens, heads), F32),
                jax.ShapeDtypeStruct((segs * heads, SEG), F32),
                jax.ShapeDtypeStruct((8, heads), F32),
            ],
            in_specs=[
                any_space, any_space, any_space, any_space,
            ],
            out_specs=[
                pl.BlockSpec((tokens, TILE), lambda i: (0, lax.rem(i + tiles, 2 * tiles))),
                pl.BlockSpec(((segs - 1) * STATE, TILE), lambda i: (0, jnp.clip(i - 2, 0, tiles - 1))),
                pl.BlockSpec((STATE, TILE), lambda i: (0, jnp.maximum(i - (LAG_Y + 2), 0))),
                any_space, any_space, any_space, any_space,
            ],
            scratch_shapes=[
                pltpu.VMEM((tokens, d_model), BF16),
                pltpu.VMEM((3, d_model, TILE), BF16),
                pltpu.VMEM((d_model, 2 * STATE + heads), BF16),
                pltpu.VMEM((1, heads), F32), pltpu.VMEM((1, heads), F32),
                pltpu.VMEM((tokens, 2 * STATE), BF16),
                pltpu.VMEM((tokens, heads), F32),
                pltpu.VMEM((segs * heads, SEG), F32),
                pltpu.VMEM((8, heads), F32),
                pltpu.SemaphoreType.DMA((2 + 2 * CHUNKS,)), pltpu.SemaphoreType.DMA((3,)), pltpu.SemaphoreType.DMA((4,)),
                pltpu.VMEM((segs * STATE, SEG), BF16),
                pltpu.VMEM((8, heads), F32),
                pltpu.VMEM((tokens, TILE), BF16),
                pltpu.VMEM((tokens, heads), F32),
                pltpu.VMEM((tokens, TILE), BF16),
                pltpu.VMEM((tiles, 8, HALF), F32),
                pltpu.VMEM((8, heads), F32),
                pltpu.VMEM((8, 8, heads), F32),
                pltpu.VMEM((tiles, 2, STATE, HALF), F32),
                pltpu.VMEM(half, F32), pltpu.VMEM(half, F32), pltpu.VMEM(half, F32),
                pltpu.VMEM(half, F32), pltpu.VMEM(half, F32), pltpu.VMEM(half, F32),
                pltpu.SemaphoreType.DMA((7,)), pltpu.SemaphoreType.DMA((8,)),
                sems, sems, sems, sems, sems, sems, sems, sems,
            ],
            compiler_params=pltpu.CompilerParams(
                dimension_semantics=("arbitrary",), collective_id=0, has_side_effects=True,
                vmem_limit_bytes=60 * 1024 * 1024),
            cost_estimate=pl.CostEstimate(flops=2 * tokens * d_model * w_in.shape[1],
                                          bytes_accessed=2 * w_in.size, transcendentals=0),
            name="project",
        )(x_loc, w_in, a_neg.reshape(1, heads), dt_bias.reshape(1, heads))

        last = tiles // 2 - 1
        return pl.pallas_call(
            mix_kernel,
            grid=(tiles // 2 + 1,),
            out_shape=jax.ShapeDtypeStruct((tokens, d_model), BF16),
            in_specs=[
                pl.BlockSpec((tokens, 2 * TILE), lambda i: (0, jnp.minimum(i, last))),
                pl.BlockSpec((tokens, 2 * TILE), lambda i: (0, jnp.minimum(i, last) + tiles // 2)),
                pl.BlockSpec(((segs - 1) * STATE, 2 * TILE), lambda i: (0, jnp.minimum(i, last))),
                pl.BlockSpec((STATE, 2 * TILE), lambda i: (0, jnp.minimum(i, last))),
                fixed((tokens, 2 * STATE)), fixed((tokens, heads)),
                fixed((segs * heads, SEG)), fixed((8, heads)), fixed((1, heads)),
                any_space, any_space,
            ],
            out_specs=any_space,
            scratch_shapes=[
                pltpu.VMEM((tokens, d_model), F32),
                pltpu.VMEM((tokens, TILE), BF16),
                pltpu.VMEM((tokens, TILE), BF16),
                pltpu.VMEM((tokens, SEG), F32),
                pltpu.VMEM((4, TILE, d_model), BF16),
                pltpu.VMEM((tokens, d_model), BF16),
                pltpu.SemaphoreType.DMA((4,)),
                pltpu.SemaphoreType.DMA(()),
                pltpu.SemaphoreType.DMA((d_model // (2 * TILE),)),
            ],
            compiler_params=pltpu.CompilerParams(
                dimension_semantics=("arbitrary",), vmem_limit_bytes=62 * 1024 * 1024),
            cost_estimate=pl.CostEstimate(flops=2 * tokens * d_model * inner,
                                          bytes_accessed=2 * w_out.size, transcendentals=0),
            name="mix",
        )(u, u, loc, h_in, bc, gl, qt, dec, d_skip.reshape(1, heads), w_out, x_loc)

    return jax.shard_map(local_mixer, mesh=mesh, in_specs=(row_spec, P(), P(), P(), P(), P()),
                         out_specs=row_spec, check_vma=False)
```
